32 devices in a mesh: group: 4 (over y, x), dev: 8 (over z, core).
Axes of the slice: x: 2, y: 2, z: 4, core: 2. Of those that a mesh axis runs over, the one named last changes fastest.
Arguments:
- node_feats: bfloat16 [8192, 1024], P(('group', 'dev')), may hold values from -60 to 60
- w_gcn: bfloat16 [1024, 1024], replicated, may hold values from -0.1875 to 0.1875
- adj_tiles: bfloat16 [64, 16, 128, 128], P(('group', 'dev')), may hold values from -0.125 to 0.125
- neighbor_blocks: int32 [64, 16], P(('group', 'dev')), may hold values from 0 to 21, all different within a row
- inner_rows: int32 [32, 8, 256], P(('group', 'dev')), may hold values from 0 to 255
- outer_rows: int32 [32, 4, 128], P(('group', 'dev')), may hold values from 0 to 255
- w_qkv: bfloat16 [1024, 3072], replicated, may hold values from -0.1875 to 0.1875
- key_blocks: int32 [64, 16], P('group'), may hold values from 0 to 15, all different within a row
- key_counts: int32 [64], P('group'), may hold values from 1 to 16
- w_out: bfloat16 [1024, 1024], replicated, may hold values from -0.1875 to 0.1875
- w_up: bfloat16 [1024, 2048], replicated, may hold values from -0.1875 to 0.1875
- w_down: bfloat16 [2048, 1024], replicated, may hold values from -0.125 to 0.125
Outputs:
- layer_out: bfloat16 [8192, 1024], P(('group', 'dev'))
The draws below stay inside these ranges and needn't reach their ends.
Inputs may be any that keep to these rules, and one draw needn't show every extreme that they name: `inner_rows`: row numbers of the sending device. `outer_rows`: row numbers of the sending device. `neighbor_blocks`: table block numbers; the 16 entries of a row differ. `key_blocks`: the 16 entries of a row differ.
All inputs are finite; a program needn't handle non-finite values.
Results may differ from the reference program's by a relative error of at most 0.012.
The reference program's roundings to bfloat16 on the way count: a program that leaves them out, or rounds other values in their place, can miss the bound.
Values may be sent and summed in bfloat16 or wider, within the bound.
No kernel may reach another device: no remote copies, remote signals or barrier semaphores. Data moves between devices by JAX's collectives and lax.ppermute only.
A program may use at most 128 MiB of HBM per device.

```python
import jax
import jax.numpy as jnp
from jax import lax

D = 1024
H = 32
HD = 32
FF = 2048
BLOCK = 128
BLK_DEV = 2
NBR = 16
KB = 16
ROWS_DEV = 256
NODES = 8192
NODE_BLKS = 64
QB_G = 16
IN_SLOT = 256
X_SLOT = 128
TAB_BLK = 22
N_GROUP = 4
N_DEV = 8
DEVICES = 32


def draw_node_feats(key, part):
    first_key = jax.random.fold_in(jax.random.fold_in(key, 11), 0)
    values = jnp.clip(jax.random.normal(first_key, (NODES, D), jnp.float32), -6.0, 6.0)
    return values.astype(jnp.bfloat16)


def set_ends(array, own_key, smallest, largest):
    dims = array.shape
    place = [jax.random.randint(jax.random.fold_in(own_key, axis), (), 0, dims[axis]) for axis in range(len(dims))]
    array = array.at[tuple(place)].set(smallest)
    longest = dims.index(max(dims))
    place[longest] = (place[longest] + 1) % dims[longest]
    return array.at[tuple(place)].set(largest)


def steps_of(rng, shape, cuts, low, top_value):
    level = 1.0
    for axis_at, shards_of in cuts:
        steps = jax.random.uniform(jax.random.fold_in(jax.random.fold_in(rng, 6), axis_at), (shards_of,), jnp.float32, low / len(cuts), top_value / len(cuts))
        level = level * jnp.repeat(jnp.exp(steps), shape[axis_at] // shards_of).reshape((-1,) + (1,) * (len(shape) - 1 - axis_at))
    return level


def picks_of(key, rows, amount, top, lift):
    ranking = jax.random.permutation(jax.random.fold_in(key, 1), amount)
    favour = ranking
    for power in range(3):
        favour = favour * favour // amount
    favour = favour * lift // amount
    tickets = jax.random.randint(jax.random.fold_in(key, 2), (rows, amount), 0, 4096) + favour
    holders = jax.random.permutation(jax.random.fold_in(key, 3), rows)[jnp.arange(amount) % rows]
    tickets = jnp.where(jnp.arange(rows)[:, None] == holders[None, :], 1 << 14, tickets)
    merit = tickets * amount + jnp.arange(amount)
    return lax.top_k(merit.astype(jnp.int32), top)[1].astype(jnp.int32)


def noise(own_key, dims, width, most, pieces=(), kind=jnp.bfloat16):
    values = jax.random.normal(own_key, dims, jnp.float32) * width
    if len(pieces) > 0:
        values = steps_of(own_key, dims, pieces, -0.22, 0.18) * values
    return jnp.clip(values, min=-most, max=most).astype(kind)


def setup_inputs(seed: int = 0) -> dict:
    arg_keys = jax.random.split(jax.random.key(seed), 13)
    return {
        "node_feats": draw_node_feats(jax.random.fold_in(arg_keys[12], 71), 0),
        "w_gcn": noise(arg_keys[1], (D, D), D ** -0.5, 0.1875),
        "adj_tiles": noise(arg_keys[2], (NODE_BLKS, NBR, BLOCK, BLOCK), (NBR * BLOCK) ** -0.5, 0.125, ((0, 32),)),
        "neighbor_blocks": picks_of(arg_keys[3], NODE_BLKS, TAB_BLK, NBR, 0),
        "inner_rows": set_ends(jax.random.randint(arg_keys[4], (DEVICES, N_DEV, IN_SLOT), 0, ROWS_DEV), jax.random.fold_in(arg_keys[4], 1), 0, ROWS_DEV - 1).astype(jnp.int32),
        "outer_rows": set_ends(jax.random.randint(arg_keys[5], (DEVICES, N_GROUP, X_SLOT), 0, ROWS_DEV), jax.random.fold_in(arg_keys[5], 1), 0, ROWS_DEV - 1).astype(jnp.int32),
        "w_qkv": noise(arg_keys[6], (D, 3 * D), D ** -0.5, 0.1875),
        "key_blocks": picks_of(arg_keys[7], (N_GROUP * QB_G), QB_G, KB, 0),
        "key_counts": set_ends(jax.random.randint(arg_keys[8], (N_GROUP * QB_G,), 1, KB + 1), jax.random.fold_in(arg_keys[8], 1), 1, KB).astype(jnp.int32),
        "w_out": noise(arg_keys[9], (D, D), D ** -0.5, 0.1875),
        "w_up": noise(arg_keys[10], (D, FF), D ** -0.5, 0.1875),
        "w_down": noise(arg_keys[11], (FF, D), FF ** -0.5, 0.125),
    }


def layer_norm(values):
    average = lax.optimization_barrier(jnp.mean(values, axis=-1, keepdims=True))
    centered = values - average
    variance = lax.optimization_barrier(jnp.mean(centered * centered, axis=-1, keepdims=True))
    return centered / jnp.sqrt(variance + 1e-05)

def reference(node_feats, w_gcn, adj_tiles, neighbor_blocks, inner_rows, outer_rows, w_qkv, key_blocks, key_counts, w_out, w_up, w_down):
    device_total = N_GROUP * N_DEV
    gcn_rows = jnp.dot(node_feats, w_gcn, preferred_element_type=jnp.float32).astype(jnp.bfloat16)
    device_ids = jnp.arange(device_total, dtype=jnp.int32)
    group_of = device_ids // N_DEV
    dev_place = device_ids % N_DEV
    own_rows = device_ids[:, None] * ROWS_DEV + jnp.arange(ROWS_DEV, dtype=jnp.int32)[None, :]
    senders = group_of[:, None] * N_DEV + jnp.arange(N_DEV, dtype=jnp.int32)[None, :]
    inner_local = inner_rows[senders, dev_place[:, None], :]
    inner_global = senders[:, :, None] * ROWS_DEV + inner_local
    far_senders = jnp.arange(N_GROUP, dtype=jnp.int32)[None, :] * N_DEV + dev_place[:, None]
    outer_local = outer_rows[far_senders, group_of[:, None], :]
    outer_global = far_senders[:, :, None] * ROWS_DEV + outer_local
    table_index = jnp.concatenate([own_rows, inner_global.reshape(device_total, -1), outer_global.reshape(device_total, -1)], axis=1).astype(jnp.int32)
    table_blocks = table_index.reshape(device_total, TAB_BLK, BLOCK)

    def aggregate(inputs):
        block_id, slots, tile_set = inputs
        owner = block_id // BLK_DEV
        source_rows = table_blocks[owner][slots]
        source = gcn_rows[source_rows]
        return jnp.einsum('sij,sjd->id', tile_set.astype(jnp.float32), source.astype(jnp.float32))
    agg = lax.map(aggregate, (jnp.arange(NODE_BLKS, dtype=jnp.int32), neighbor_blocks, adj_tiles))
    agg = agg.reshape(NODES, D)
    features = node_feats.astype(jnp.float32)
    local_branch = layer_norm(features + agg)
    qkv = jnp.dot(node_feats, w_qkv, preferred_element_type=jnp.float32).astype(jnp.bfloat16)
    query_blocks = qkv[:, :D].reshape(NODE_BLKS, BLOCK, H, HD)
    key_rows = qkv[:, D:2 * D].reshape(NODE_BLKS, BLOCK, H, HD)
    value_rows = qkv[:, 2 * D:].reshape(NODE_BLKS, BLOCK, H, HD)
    scale = 1.0 / HD ** 0.5

    def attend(inputs):
        block_ids, picks, counts = inputs
        base = block_ids // QB_G * QB_G
        chosen = (base[:, None] + picks).astype(jnp.int32)
        queries = query_blocks[block_ids].astype(jnp.float32)
        keys_here = key_rows[chosen].astype(jnp.float32)
        values_here = value_rows[chosen].astype(jnp.float32)
        scores = jnp.einsum('qihe,qsjhe->qhisj', queries, keys_here) * scale
        live = jnp.arange(KB, dtype=jnp.int32)[None, :] < counts[:, None]
        scores = jnp.where(live[:, None, None, :, None], scores, -jnp.inf)
        highest = lax.optimization_barrier(jnp.max(scores, axis=(3, 4), keepdims=True))
        expos = jnp.exp(scores - highest)
        totals = lax.optimization_barrier(jnp.sum(expos, axis=(3, 4), keepdims=True))
        probs = (expos / totals).astype(jnp.bfloat16)
        mixed = jnp.einsum('qhisj,qsjhe->qihe', probs.astype(jnp.float32), values_here)
        return mixed.astype(jnp.bfloat16)
    steps_total = NODE_BLKS // 4
    attended = lax.map(attend, (jnp.arange(NODE_BLKS, dtype=jnp.int32).reshape(steps_total, 4), key_blocks.reshape(steps_total, 4, KB), key_counts.reshape(steps_total, 4)))
    attended = attended.reshape(NODES, D)
    attn_branch = layer_norm(features + jnp.dot(attended, w_out, preferred_element_type=jnp.float32))
    summed = local_branch + attn_branch
    summed_in = summed.astype(jnp.bfloat16)
    activated = jax.nn.gelu(jnp.dot(summed_in, w_up, preferred_element_type=jnp.float32)).astype(jnp.bfloat16)
    layer_out = layer_norm(summed + jnp.dot(activated, w_down, preferred_element_type=jnp.float32))
    return layer_out.astype(jnp.bfloat16)
```

```python
import functools
import math

import jax
import jax.numpy as jnp
from jax import lax
from jax.experimental import pallas as pl
from jax.experimental.pallas import tpu as pltpu
from jax.sharding import PartitionSpec as P

H = 32
LOW = -1e30
CORES = 2


def layer_norm(values):
    average = jnp.mean(values, axis=-1, keepdims=True)
    centered = values - average
    variance = jnp.mean(centered * centered, axis=-1, keepdims=True)
    return centered / jnp.sqrt(variance + 1e-05)


def gathered_plan(
    node_feats,
    w_gcn,
    adj_tiles,
    neighbor_blocks,
    inner_rows,
    outer_rows,
    w_qkv,
    key_blocks,
    key_counts,
    w_out,
    w_up,
    w_down,
):
    row_count = node_feats.shape[0]
    width = node_feats.shape[1]
    block_rows = adj_tiles.shape[-1]
    peers = lax.axis_size("dev")
    clusters = lax.axis_size("group")
    head_size = width // H
    local_heads = H // peers
    head_cols = local_heads * head_size
    gcn_rows = jnp.dot(node_feats, w_gcn, preferred_element_type=jnp.float32).astype(jnp.bfloat16)
    qkv_split = jnp.einsum(
        "rd,dtph->pthr",
        node_feats,
        w_qkv.reshape(width, 3, peers, head_cols),
        preferred_element_type=jnp.float32,
    ).astype(jnp.bfloat16)
    whole_rows, whole_lists = (
        lax.all_gather(gcn_rows, "dev", axis=0, tiled=True),
        lax.all_gather(inner_rows, "dev", axis=0, tiled=True),
    )
    chosen_lists = lax.dynamic_index_in_dim(
        whole_lists, lax.axis_index("dev"), axis=1, keepdims=False
    )
    inner_index = (jnp.arange(peers, dtype=jnp.int32)[:, None] * row_count + chosen_lists).reshape(
        -1
    )
    inner_part = whole_rows[inner_index]
    far_rows, far_lists = (
        lax.all_gather(gcn_rows, "group", axis=0, tiled=True),
        lax.all_gather(outer_rows, "group", axis=0, tiled=True),
    )
    chosen_far = lax.dynamic_index_in_dim(
        far_lists, lax.axis_index("group"), axis=1, keepdims=False
    )
    outer_index = (jnp.arange(clusters, dtype=jnp.int32)[:, None] * row_count + chosen_far).reshape(
        -1
    )
    outer_part = far_rows[outer_index]
    head_parts = lax.all_to_all(qkv_split, "dev", split_axis=0, concat_axis=3, tiled=True)
    table = jnp.concatenate([gcn_rows, inner_part, outer_part], axis=0)
    table_count = table.shape[0] // block_rows
    selector = (
        neighbor_blocks[:, :, None] == jnp.arange(table_count, dtype=jnp.int32)[None, None, :]
    ).astype(jnp.bfloat16)
    spread = jnp.einsum(
        "bst,bsij->bitj", selector, adj_tiles, preferred_element_type=jnp.float32
    ).astype(jnp.bfloat16)
    agg = jnp.dot(
        spread.reshape(row_count, table_count * block_rows),
        table,
        preferred_element_type=jnp.float32,
    )
    features = node_feats.astype(jnp.float32)
    local_branch = layer_norm(features + agg)
    group_rows = row_count * peers
    block_total = group_rows // block_rows
    per_step = 8
    steps_total = block_total // per_step
    head_parts = head_parts.reshape(3, local_heads, head_size, block_total, block_rows)
    query_part = (
        head_parts[0]
        .reshape(local_heads, head_size, steps_total, per_step, block_rows)
        .transpose(2, 0, 1, 3, 4)
    )
    key_value = head_parts[1:3]
    scale = 1.0 / head_size**0.5
    slot_count = key_blocks.shape[1]

    def attend(inputs):
        picks, counts, queries = inputs
        picker = (
            picks[:, :, None] == jnp.arange(block_total, dtype=jnp.int32)[None, None, :]
        ).astype(jnp.bfloat16)
        picked = jnp.einsum(
            "qst,kletj->kleqsj", picker, key_value, preferred_element_type=jnp.float32
        ).astype(jnp.bfloat16)
        keys_here = picked[0]
        values_here = picked[1]
        scores = (
            jnp.einsum("leqi,leqsj->qlisj", queries, keys_here, preferred_element_type=jnp.float32)
            * scale
        )
        live = jnp.arange(slot_count, dtype=jnp.int32)[None, :] < counts[:, None]
        scores = jnp.where(live[:, None, None, :, None], scores, -jnp.inf)
        highest = jnp.max(scores, axis=(3, 4), keepdims=True)
        expos = jnp.exp(scores - highest)
        totals = jnp.sum(expos, axis=(3, 4), keepdims=True)
        probs = (expos / totals).astype(jnp.bfloat16)
        mixed = jnp.einsum(
            "qlisj,leqsj->leqi", probs, values_here, preferred_element_type=jnp.float32
        )
        return mixed.astype(jnp.bfloat16)

    attended = lax.map(
        attend,
        (
            key_blocks.reshape(steps_total, per_step, slot_count),
            key_counts.reshape(steps_total, per_step),
            query_part,
        ),
    )
    attended = attended.transpose(1, 2, 0, 3, 4).reshape(head_cols, group_rows)
    returned = lax.all_to_all(attended, "dev", split_axis=1, concat_axis=0, tiled=True)
    projected = lax.dot_general(
        returned, w_out, (((0,), (0,)), ((), ())), preferred_element_type=jnp.float32
    )
    attn_branch = layer_norm(features + projected)
    summed = local_branch + attn_branch
    summed_in = summed.astype(jnp.bfloat16)
    activated = jax.nn.gelu(jnp.dot(summed_in, w_up, preferred_element_type=jnp.float32)).astype(
        jnp.bfloat16
    )
    layer_out = layer_norm(summed + jnp.dot(activated, w_down, preferred_element_type=jnp.float32))
    return layer_out.astype(jnp.bfloat16)


BF = jnp.bfloat16
F32 = jnp.float32
SMEM = pl.BlockSpec(memory_space=pltpu.SMEM)
VMEM = pl.BlockSpec(memory_space=pltpu.VMEM)


def mm(a, b, dims):
    return lax.dot_general(a, b, (dims, ((), ())), preferred_element_type=F32)


def attend_kernel(first, sources, rows, block, heads_step, scale, *refs):
    info, key_blocks, key_counts, *refs = refs
    if first:
        own, partner, wq, wk, wv, qt_ref, max_ref, sum_ref, acc_ref, live_ref = refs
        pieces = [own]
    else:
        pieces = refs[:sources]
        wk, wv, qt_in, max_in, sum_in, acc_in, max_ref, sum_ref, acc_ref, live_ref = refs[sources:]
    per_dev = rows // block
    slots = key_blocks.shape[1]
    chip = info[0]
    width_step = wk.shape[1]
    head = width_step // heads_step
    packed = 128 // head
    queries = CORES * rows

    @pl.when(pl.program_id(0) == 0)
    def _():
        for p in range(len(pieces)):
            for j in range(per_dev):
                wanted = info[1 + p] * per_dev + j
                for i in range(CORES * per_dev):
                    at = info[8 + i]
                    count = key_counts[at]
                    hit = jnp.int32(0)
                    for s in range(slots):
                        hit = jnp.where((key_blocks[at, s] == wanted) & (s < count), 1, hit)
                    live_ref[(p * per_dev + j) * CORES * per_dev + i] = hit

    if first:
        q_own = mm(own[0:rows, :], wq[...], ((1,), (0,))).astype(BF)
        q_par = mm(partner[0:rows, :], wq[...], ((1,), (0,))).astype(BF)
        qt_ref[:, 0:rows] = q_own.T
        qt_ref[:, rows:queries] = q_par.T
        max_ref[...] = jnp.full(max_ref.shape, LOW, F32)
        sum_ref[...] = jnp.zeros(sum_ref.shape, F32)
        acc_ref[...] = jnp.zeros(acc_ref.shape, F32)
        qt = qt_ref
    else:
        max_ref[...] = max_in[...]
        sum_ref[...] = sum_in[...]
        acc_ref[...] = acc_in[...]
        qt = qt_in
    belongs = lax.broadcasted_iota(jnp.int32, (128, queries), 0) // head

    for p, piece in enumerate(pieces):

        @pl.when(info[1 + sources + p] != 0)
        def _(p=p, piece=piece):
            x = piece[0:rows, :]
            keys = mm(x, wk[...], ((1,), (0,))).astype(BF)
            values = mm(x, wv[...], ((1,), (0,))).astype(BF).T
            alive = []
            for j in range(per_dev):
                base = (p * per_dev + j) * CORES * per_dev
                alive.append(
                    jnp.concatenate(
                        [
                            jnp.full((1, block), live_ref[base + i], jnp.int32)
                            for i in range(CORES * per_dev)
                        ],
                        axis=1,
                    )
                    != 0
                )
            ones = jnp.ones((16, rows), BF)
            for h in range(heads_step):
                lane = (h // packed) * 128
                q_head = jnp.where(belongs == h % packed, qt[lane : lane + 128, :], 0).astype(BF)
                scores = mm(keys[:, lane : lane + 128], q_head, ((1,), (0,)))
                parts = [scores[j * block : (j + 1) * block] for j in range(per_dev)]
                top = max_ref[h : h + 1, :]
                new_top = top
                for j in range(per_dev):
                    peak = jnp.max(parts[j], axis=0, keepdims=True) * scale
                    new_top = jnp.maximum(new_top, jnp.where(alive[j], peak, LOW))
                probs = jnp.concatenate(
                    [
                        jnp.exp2(parts[j] * scale - jnp.where(alive[j], new_top, -LOW))
                        for j in range(per_dev)
                    ],
                    axis=0,
                ).astype(BF)
                left = jnp.concatenate([values[h * head : (h + 1) * head, :], ones], axis=0)
                mixed = mm(left, probs, ((1,), (0,)))
                fade = jnp.exp2(top - new_top)
                max_ref[h : h + 1, :] = new_top
                sum_ref[h : h + 1, :] = sum_ref[h : h + 1, :] * fade + mixed[head : head + 1, :]
                at = slice(h * head, (h + 1) * head)
                acc_ref[at, :] = acc_ref[at, :] * fade + mixed[0:head, :]


def attend_call(first, pieces, state, info, key_blocks, key_counts, w_qkv, rows, block, name):
    width = pieces[0].shape[1]
    head = width // H
    step = 256
    groups = width // step
    heads_step = step // head
    queries = CORES * rows
    whole = lambda a: pl.BlockSpec(a.shape, lambda g: (0,) * a.ndim)
    weight = lambda part: pl.BlockSpec((width, step), lambda g, part=part: (0, part * groups + g))
    tall = pl.BlockSpec((step, queries), lambda g: (g, 0))
    small = pl.BlockSpec((heads_step, queries), lambda g: (g, 0))
    shapes = [
        jax.ShapeDtypeStruct((H, queries), F32),
        jax.ShapeDtypeStruct((H, queries), F32),
        jax.ShapeDtypeStruct((width, queries), F32),
    ]
    count = 1 if first else len(pieces)
    scale = math.log2(math.e) / math.sqrt(head)
    kernel = functools.partial(attend_kernel, first, count, rows, block, heads_step, scale)
    if first:
        in_specs = [SMEM] * 3 + [whole(p) for p in pieces] + [weight(0), weight(1), weight(2)]
        out_specs = [tall, small, small, tall]
        out_shape = [jax.ShapeDtypeStruct((width, queries), BF)] + shapes
        args = [info, key_blocks, key_counts, *pieces, w_qkv, w_qkv, w_qkv]
        aliases = {}
    else:
        qt, top, total, acc = state
        in_specs = (
            [SMEM] * 3 + [whole(p) for p in pieces] + [weight(1), weight(2), tall, small, small, tall]
        )
        out_specs = [small, small, tall]
        out_shape = shapes
        args = [info, key_blocks, key_counts, *pieces, w_qkv, w_qkv, qt, top, total, acc]
        at = 3 + len(pieces) + 3
        aliases = {at: 0, at + 1: 1, at + 2: 2}
    flops = count * (2 * rows * width * 2 * width + 4 * rows * queries * width * 4)
    out = pl.pallas_call(
        kernel,
        grid=(groups,),
        in_specs=in_specs,
        out_specs=out_specs,
        out_shape=out_shape,
        scratch_shapes=[pltpu.SMEM((count * (rows // block) * CORES * (rows // block),), jnp.int32)],
        input_output_aliases=aliases,
        cost_estimate=pl.CostEstimate(
            flops=flops, transcendentals=count * H * rows * queries, bytes_accessed=4 << 20
        ),
        name=name,
    )(*args)
    if first:
        return tuple(out)
    return (state[0], *out)


def pick_row(tile, at):
    rows = lax.broadcasted_iota(jnp.int32, tile.shape, 0)
    return jnp.sum(jnp.where(rows == at, tile.astype(F32), 0.0), axis=0, keepdims=True)


def add_pieces(info, base, pieces, spread, y_own, y_par, rows, slot, block, blocks_of):
    numbers = lax.broadcasted_iota(jnp.int32, (rows, slot), 0).astype(F32)
    for p, piece in enumerate(pieces):

        @pl.when(info[base + len(pieces) + p] != 0)
        def _(p=p, piece=piece):
            lists = piece[rows:, 0:slot]
            for dest, target in ((0, y_own), (1, y_par)):
                row = pick_row(lists, info[6 + dest])
                chosen = jnp.where(numbers == row, 1.0, 0.0).astype(BF)
                mix = jnp.zeros((rows, rows), F32)
                for j in range(slot // block):
                    tile = spread(dest, p, j)
                    mix = mix + mm(tile, chosen[:, j * block : (j + 1) * block], ((1,), (1,)))
                target[...] += mm(mix.astype(BF), piece[0:rows, :], ((1,), (0,)))


def gather_kernel(count, far_count, rows, slot, far_slot, block, *refs):
    info, nb_own, nb_par, own, adj_own, adj_par, *refs = refs
    pieces = refs[:count]
    far = refs[count : count + far_count]
    y_own, y_par, spread = refs[count + far_count :]
    spread[...] = jnp.zeros(spread.shape, BF)
    per_dev, tiles = adj_own.shape[0], adj_own.shape[1]
    for dest, (adj, nb) in enumerate(((adj_own, nb_own), (adj_par, nb_par))):
        for b in range(per_dev):
            for s in range(tiles):
                spread[dest, nb[b, s], b * block : (b + 1) * block, :] = adj[b, s]
    total = jnp.zeros(y_own.shape, F32)
    for j in range(rows // block):
        total = total + mm(spread[0, j], own[j * block : (j + 1) * block, :], ((1,), (0,)))
    first_far = rows // block + info[5] * (slot // block)
    for f in range(far_count):
        for j in range(far_slot // block):
            source = info[10 + 2 * count + f]
            tile = spread[0, first_far + source * (far_slot // block) + j]
            total = total + mm(tile, far[f][j * block : (j + 1) * block, :], ((1,), (0,)))
    y_own[...] = total
    y_par[...] = jnp.zeros(y_par.shape, F32)

    def tile_of(dest, p, j):
        return spread[dest, rows // block + info[10 + p] * (slot // block) + j]

    add_pieces(info, 10, pieces, tile_of, y_own, y_par, rows, slot, block, None)


def gather_more_kernel(count, rows, slot, block, *refs):
    info, *refs = refs
    pieces = refs[:count]
    tiles = refs[count : 2 * count]
    own_in, par_in, y_own, y_par = refs[2 * count :]
    y_own[...] = own_in[...]
    y_par[...] = par_in[...]

    def tile_of(dest, p, j):
        return tiles[p][dest, j]

    add_pieces(info, 10, pieces, tile_of, y_own, y_par, rows, slot, block, None)


def local_kernel(x, y_own, y_got, w, out):
    mixed = (y_own[...] + y_got[...]).astype(BF)
    agg = mm(mixed, w[...], ((1,), (0,)))
    out[...] = layer_norm(x[...].astype(F32) + agg)


def tail_kernel(rows, x, local, top, total, acc, got, got_stats, w_out, w_up, w_down, out, wo, wu, wd, sems):
    loads = [
        pltpu.make_async_copy(src, dst, sems.at[i])
        for i, (src, dst) in enumerate(((w_out, wo), (w_up, wu), (w_down, wd)))
    ]
    for load in loads:
        load.start()
    heads = top.shape[0]
    width = acc.shape[0]
    head = width // heads
    top_a = top[:, 0:rows]
    top_b = got_stats[0:heads, :]
    peak = jnp.maximum(top_a, top_b)
    fade_a = jnp.exp2(top_a - peak)
    fade_b = jnp.exp2(top_b - peak)
    whole = total[:, 0:rows] * fade_a + got_stats[heads : 2 * heads, :] * fade_b
    fade_a = fade_a / whole
    fade_b = fade_b / whole
    pieces = []
    for h in range(heads):
        at = slice(h * head, (h + 1) * head)
        pieces.append(
            (
                acc[at, 0:rows] * fade_a[h : h + 1, :]
                + got[at, :].astype(F32) * fade_b[h : h + 1, :]
            ).astype(BF)
        )
    attended = jnp.concatenate(pieces, axis=0)
    loads[0].wait()
    projected = mm(attended, wo[...], ((0,), (0,)))
    summed = local[...] + layer_norm(x[...].astype(F32) + projected)
    loads[1].wait()
    activated = jax.nn.gelu(mm(summed.astype(BF), wu[...], ((1,), (0,)))).astype(BF)
    loads[2].wait()
    out[...] = layer_norm(summed + mm(activated, wd[...], ((1,), (0,)))).astype(BF)


def line_plan(
    node_feats,
    w_gcn,
    adj_tiles,
    neighbor_blocks,
    inner_rows,
    outer_rows,
    w_qkv,
    key_blocks,
    key_counts,
    w_out,
    w_up,
    w_down,
):
    rows, width = node_feats.shape
    block = adj_tiles.shape[-1]
    per_dev = rows // block
    peers = lax.axis_size("dev")
    clusters = lax.axis_size("group")
    chips = peers // CORES
    slot = inner_rows.shape[-1]
    far_slot = outer_rows.shape[-1]
    me = lax.axis_index("dev")
    cluster = lax.axis_index("group")
    core = me % CORES
    mate = me + 1 - 2 * core

    swap = [(CORES * c + k, CORES * c + 1 - k) for c in range(chips) for k in range(CORES)]

    def hop(value, step, far):
        pairs = []
        for c in range(chips):
            to = c + step
            if 0 <= to < chips and 0 <= to - step * far < chips:
                pairs += [(CORES * c + k, CORES * to + k) for k in range(CORES)]
        return lax.ppermute(value, "dev", pairs)

    lists = jnp.pad(inner_rows[0].astype(BF), ((0, 0), (0, width - slot)))
    piece = jnp.concatenate([node_feats, lists], axis=0)
    left, right = hop(piece, 1, 1), hop(piece, -1, 1)
    mate_piece = lax.ppermute(piece, "dev", swap)
    mate_adj = lax.ppermute(adj_tiles, "dev", swap)
    mate_nb = lax.ppermute(neighbor_blocks, "dev", swap)

    numbers = jnp.arange(rows, dtype=jnp.int32)
    chosen = (outer_rows[0].reshape(-1)[:, None] == numbers[None, :]).astype(BF)
    picked = jnp.dot(chosen, node_feats, preferred_element_type=F32).astype(BF)
    picked = picked.reshape(clusters, far_slot, width)
    far = [lax.dynamic_index_in_dim(picked, cluster, 0, keepdims=False)]
    far_from = [cluster]
    for s in range(1, clusters):
        if clusters & (clusters - 1) == 0:
            pairs = [(c, c ^ s) for c in range(clusters)]
            to, source = cluster ^ s, cluster ^ s
        else:
            pairs = [(c, (c + s) % clusters) for c in range(clusters)]
            to, source = (cluster + s) % clusters, (cluster - s) % clusters
        sent = lax.dynamic_index_in_dim(picked, to, 0, keepdims=False)
        far.append(lax.ppermute(sent, "group", pairs))
        far_from.append(source)

    blocks_at = [me * per_dev + b for b in range(per_dev)] + [mate * per_dev + b for b in range(per_dev)]

    def info_of(sources):
        flags = [(s >= 0) & (s < peers) for s in sources]
        clipped = [jnp.clip(s, 0, peers - 1) for s in sources]
        return clipped, flags

    def pack(entries):
        return jnp.stack([jnp.asarray(e).astype(jnp.int32) for e in entries])

    def attend_info(sources):
        clipped, flags = info_of(sources)
        entries = [me // CORES, *clipped, *flags]
        entries += [0] * (8 - len(entries)) + blocks_at
        return pack(entries)

    def gather_info(sources):
        clipped, flags = info_of(sources)
        return pack([0, 0, 0, 0, 0, peers, me, mate, 0, 0, *clipped, *flags, *far_from])

    state = attend_call(
        True, [piece, mate_piece], None, attend_info([me]), key_blocks, key_counts, w_qkv, rows, block, "attend0"
    )
    arrived, origin = [piece], [me]
    for step in range(1, chips):
        pair, sources = [left, right], [me - CORES * step, me + CORES * step]
        if step + 1 < chips:
            left, right = hop(left, 1, step + 1), hop(right, -1, step + 1)
        if step + 1 == chips:
            sums = gather_call(
                arrived, gather_info(origin), node_feats, adj_tiles, mate_adj, neighbor_blocks, mate_nb,
                far, rows, slot, far_slot, block,
            )
            sums = gather_more_call(pair, gather_info(sources), sums, rows, slot, block)
            y_got = lax.ppermute(sums[1], "dev", swap)
        state = attend_call(
            False, pair, state, attend_info(sources), key_blocks, key_counts, w_qkv, rows, block, f"attend{step}"
        )
        arrived += pair
        origin += sources
    _, top, total, acc = state
    got = lax.ppermute(acc[:, rows:], "dev", swap)
    stats = jnp.concatenate([top[:, rows:], total[:, rows:]], axis=0)
    got_stats = lax.ppermute(stats, "dev", swap)
    local = pl.pallas_call(
        local_kernel,
        in_specs=[VMEM] * 4,
        out_specs=VMEM,
        out_shape=jax.ShapeDtypeStruct((rows, width), F32),
        cost_estimate=pl.CostEstimate(flops=2 * rows * width * width, transcendentals=0, bytes_accessed=4 << 20),
        name="local",
    )(node_feats, sums[0], y_got, w_gcn)
    hbm = pl.BlockSpec(memory_space=pl.ANY)
    return pl.pallas_call(
        functools.partial(tail_kernel, rows),
        in_specs=[VMEM] * 7 + [hbm] * 3,
        out_specs=VMEM,
        out_shape=jax.ShapeDtypeStruct((rows, width), BF),
        scratch_shapes=[
            pltpu.VMEM(w_out.shape, BF),
            pltpu.VMEM(w_up.shape, BF),
            pltpu.VMEM(w_down.shape, BF),
            pltpu.SemaphoreType.DMA((3,)),
        ],
        cost_estimate=pl.CostEstimate(
            flops=2 * rows * width * (width + 2 * w_up.shape[1]), transcendentals=0, bytes_accessed=12 << 20
        ),
        name="tail",
    )(node_feats, local, top, total, acc, got, got_stats, w_out, w_up, w_down)


def gather_call(
    pieces, info, own, adj_own, adj_par, nb_own, nb_par, far, rows, slot, far_slot, block
):
    width = own.shape[1]
    table_blocks = rows // block + (int(lax.axis_size("dev")) * slot + len(far) * far_slot) // block
    y = jax.ShapeDtypeStruct((rows, width), F32)
    spread = jax.ShapeDtypeStruct((CORES, table_blocks, rows, block), BF)
    return pl.pallas_call(
        functools.partial(gather_kernel, len(pieces), len(far), rows, slot, far_slot, block),
        in_specs=[SMEM] * 3 + [VMEM] * (3 + len(pieces) + len(far)),
        out_specs=[VMEM] * 3,
        out_shape=[y, y, spread],
        cost_estimate=pl.CostEstimate(
            flops=2 * rows * rows * width * (2 * len(pieces)), transcendentals=0, bytes_accessed=8 << 20
        ),
        name="gather",
    )(info, nb_own, nb_par, own, adj_own, adj_par, *pieces, *far)


def gather_more_call(pieces, info, sums, rows, slot, block):
    y_own, y_par, spread = sums
    each = slot // block
    count = len(pieces)
    base = rows // block // each
    tile = [
        pl.BlockSpec(
            (CORES, each, rows, block), lambda i, info, p=p: (0, base + info[10 + p], 0, 0)
        )
        for p in range(count)
    ]
    whole = lambda a: pl.BlockSpec(a.shape, lambda i, info: (0,) * a.ndim)
    out = pl.pallas_call(
        functools.partial(gather_more_kernel, count, rows, slot, block),
        grid_spec=pltpu.PrefetchScalarGridSpec(
            num_scalar_prefetch=1,
            grid=(1,),
            in_specs=[whole(p) for p in pieces] + tile + [whole(y_own), whole(y_par)],
            out_specs=[whole(y_own), whole(y_par)],
        ),
        out_shape=[jax.ShapeDtypeStruct(y_own.shape, F32)] * 2,
        input_output_aliases={1 + 2 * count: 0, 2 + 2 * count: 1},
        cost_estimate=pl.CostEstimate(
            flops=4 * rows * rows * y_own.shape[1] * count, transcendentals=0, bytes_accessed=4 << 20
        ),
        name="gather_more",
    )(info, *pieces, *([spread] * count), y_own, y_par)
    return out


def per_device(*args):
    inner, feats, tiles = args[4], args[0], args[2]
    whole_slots = inner.shape[-1] == feats.shape[0] and feats.shape[0] <= 256
    if whole_slots and lax.axis_size("dev") % CORES == 0 and inner.shape[-1] % tiles.shape[-1] == 0:
        return line_plan(*args)
    return gathered_plan(*args)


def solution(mesh):
    placed = (
        P(("group", "dev"), None),
        P(),
        P(("group", "dev"), None, None, None),
        P(("group", "dev"), None),
        P(("group", "dev"), None, None),
        P(("group", "dev"), None, None),
        P(),
        P("group", None),
        P("group"),
        P(),
        P(),
        P(),
    )
    return jax.shard_map(
        per_device, mesh=mesh, in_specs=placed, out_specs=P(("group", "dev"), None), check_vma=False
    )
```

```python
import functools
import math

import jax
import jax.numpy as jnp
from jax import lax
from jax.experimental import pallas as pl
from jax.experimental.pallas import tpu as pltpu
from jax.sharding import PartitionSpec as P

H = 32
LOW = -1e30
CORES = 2


def layer_norm(values):
    average = jnp.mean(values, axis=-1, keepdims=True)
    centered = values - average
    variance = jnp.mean(centered * centered, axis=-1, keepdims=True)
    return centered / jnp.sqrt(variance + 1e-05)


def gathered_plan(
    node_feats,
    w_gcn,
    adj_tiles,
    neighbor_blocks,
    inner_rows,
    outer_rows,
    w_qkv,
    key_blocks,
    key_counts,
    w_out,
    w_up,
    w_down,
):
    row_count = node_feats.shape[0]
    width = node_feats.shape[1]
    block_rows = adj_tiles.shape[-1]
    peers = lax.axis_size("dev")
    clusters = lax.axis_size("group")
    head_size = width // H
    local_heads = H // peers
    head_cols = local_heads * head_size
    gcn_rows = jnp.dot(node_feats, w_gcn, preferred_element_type=jnp.float32).astype(jnp.bfloat16)
    qkv_split = jnp.einsum(
        "rd,dtph->pthr",
        node_feats,
        w_qkv.reshape(width, 3, peers, head_cols),
        preferred_element_type=jnp.float32,
    ).astype(jnp.bfloat16)
    whole_rows, whole_lists = (
        lax.all_gather(gcn_rows, "dev", axis=0, tiled=True),
        lax.all_gather(inner_rows, "dev", axis=0, tiled=True),
    )
    chosen_lists = lax.dynamic_index_in_dim(
        whole_lists, lax.axis_index("dev"), axis=1, keepdims=False
    )
    inner_index = (jnp.arange(peers, dtype=jnp.int32)[:, None] * row_count + chosen_lists).reshape(
        -1
    )
    inner_part = whole_rows[inner_index]
    far_rows, far_lists = (
        lax.all_gather(gcn_rows, "group", axis=0, tiled=True),
        lax.all_gather(outer_rows, "group", axis=0, tiled=True),
    )
    chosen_far = lax.dynamic_index_in_dim(
        far_lists, lax.axis_index("group"), axis=1, keepdims=False
    )
    outer_index = (jnp.arange(clusters, dtype=jnp.int32)[:, None] * row_count + chosen_far).reshape(
        -1
    )
    outer_part = far_rows[outer_index]
    head_parts = lax.all_to_all(qkv_split, "dev", split_axis=0, concat_axis=3, tiled=True)
    table = jnp.concatenate([gcn_rows, inner_part, outer_part], axis=0)
    table_count = table.shape[0] // block_rows
    selector = (
        neighbor_blocks[:, :, None] == jnp.arange(table_count, dtype=jnp.int32)[None, None, :]
    ).astype(jnp.bfloat16)
    spread = jnp.einsum(
        "bst,bsij->bitj", selector, adj_tiles, preferred_element_type=jnp.float32
    ).astype(jnp.bfloat16)
    agg = jnp.dot(
        spread.reshape(row_count, table_count * block_rows),
        table,
        preferred_element_type=jnp.float32,
    )
    features = node_feats.astype(jnp.float32)
    local_branch = layer_norm(features + agg)
    group_rows = row_count * peers
    block_total = group_rows // block_rows
    per_step = 8
    steps_total = block_total // per_step
    head_parts = head_parts.reshape(3, local_heads, head_size, block_total, block_rows)
    query_part = (
        head_parts[0]
        .reshape(local_heads, head_size, steps_total, per_step, block_rows)
        .transpose(2, 0, 1, 3, 4)
    )
    key_value = head_parts[1:3]
    scale = 1.0 / head_size**0.5
    slot_count = key_blocks.shape[1]

    def attend(inputs):
        picks, counts, queries = inputs
        picker = (
            picks[:, :, None] == jnp.arange(block_total, dtype=jnp.int32)[None, None, :]
        ).astype(jnp.bfloat16)
        picked = jnp.einsum(
            "qst,kletj->kleqsj", picker, key_value, preferred_element_type=jnp.float32
        ).astype(jnp.bfloat16)
        keys_here = picked[0]
        values_here = picked[1]
        scores = (
            jnp.einsum("leqi,leqsj->qlisj", queries, keys_here, preferred_element_type=jnp.float32)
            * scale
        )
        live = jnp.arange(slot_count, dtype=jnp.int32)[None, :] < counts[:, None]
        scores = jnp.where(live[:, None, None, :, None], scores, -jnp.inf)
        highest = jnp.max(scores, axis=(3, 4), keepdims=True)
        expos = jnp.exp(scores - highest)
        totals = jnp.sum(expos, axis=(3, 4), keepdims=True)
        probs = (expos / totals).astype(jnp.bfloat16)
        mixed = jnp.einsum(
            "qlisj,leqsj->leqi", probs, values_here, preferred_element_type=jnp.float32
        )
        return mixed.astype(jnp.bfloat16)

    attended = lax.map(
        attend,
        (
            key_blocks.reshape(steps_total, per_step, slot_count),
            key_counts.reshape(steps_total, per_step),
            query_part,
        ),
    )
    attended = attended.transpose(1, 2, 0, 3, 4).reshape(head_cols, group_rows)
    returned = lax.all_to_all(attended, "dev", split_axis=1, concat_axis=0, tiled=True)
    projected = lax.dot_general(
        returned, w_out, (((0,), (0,)), ((), ())), preferred_element_type=jnp.float32
    )
    attn_branch = layer_norm(features + projected)
    summed = local_branch + attn_branch
    summed_in = summed.astype(jnp.bfloat16)
    activated = jax.nn.gelu(jnp.dot(summed_in, w_up, preferred_element_type=jnp.float32)).astype(
        jnp.bfloat16
    )
    layer_out = layer_norm(summed + jnp.dot(activated, w_down, preferred_element_type=jnp.float32))
    return layer_out.astype(jnp.bfloat16)


BF = jnp.bfloat16
F32 = jnp.float32
SMEM = pl.BlockSpec(memory_space=pltpu.SMEM)
VMEM = pl.BlockSpec(memory_space=pltpu.VMEM)
GROUP_COLS = 256
DEPTH = 3


def mm(a, b, dims=((1,), (0,))):
    return lax.dot_general(a, b, (dims, ((), ())), preferred_element_type=F32)


def grant(mib):
    return pltpu.CompilerParams(vmem_limit_bytes=mib << 20)


def sources_of(step, me, peers):
    left, right = me - CORES * step, me + CORES * step
    return left, right, left >= 0, right < peers


def attend_kernel(mode, step, rows, block, peers, where, live, *refs):
    first, last, both = mode
    if first:
        own, mate_piece, w, qt_ref, max_ref, sum_ref, acc_ref, score_ref, prob_ref = refs
    else:
        left_piece, right_piece, w, qt_ref, max_in, sum_in, acc_in, *refs = refs
        if last:
            send_ref, *refs = refs
        max_ref, sum_ref, acc_ref, score_ref, prob_ref = refs
    width = w.shape[0]
    head = width // H
    heads_step = GROUP_COLS // head
    per_dev = rows // block
    queries = CORES * rows
    scale = math.log2(math.e) / math.sqrt(head)
    me = where[0]
    mate = me + 1 - 2 * (me % CORES)
    if first:
        source, needed = me, None
    else:
        left, right, has_left, has_right = sources_of(step, me, peers)
        if both:
            source, needed = right, has_left & has_right
        else:
            source, needed = jnp.where(has_left, left, right), has_left | has_right

    def run():
        if first:
            x = own[0:rows, :]
        elif both:
            x = right_piece[0:rows, :]
        else:
            x = jnp.where(has_left, left_piece[0:rows, :], right_piece[0:rows, :])
        query_blocks = [dev * per_dev + b for dev in (me, mate) for b in range(per_dev)]
        alive = []
        for j in range(per_dev):
            bit = source * per_dev + j
            flags = [jnp.full((1, block), (live[q] >> bit) & 1, jnp.int32) for q in query_blocks]
            alive.append(jnp.concatenate(flags, axis=1) != 0)
        ones = jnp.ones((16, rows), BF)

        def group(g, carry):
            cols = pl.multiple_of(g * GROUP_COLS, GROUP_COLS)
            heads_at = pl.multiple_of(g * heads_step, heads_step)

            def weight(part):
                return w[:, pl.ds(pl.multiple_of(part * width + cols, GROUP_COLS), GROUP_COLS)]

            if first:
                wq = weight(0)
                qt_ref[pl.ds(cols, GROUP_COLS), 0:rows] = mm(x, wq).astype(BF).T
                mate_q = mm(mate_piece[0:rows, :], wq).astype(BF)
                qt_ref[pl.ds(cols, GROUP_COLS), rows:queries] = mate_q.T
                tops = jnp.full((heads_step, queries), LOW, F32)
                sums = jnp.zeros((heads_step, queries), F32)
            else:
                tops = max_in[pl.ds(heads_at, heads_step), :]
                sums = sum_in[pl.ds(heads_at, heads_step), :]
            keys = mm(x, weight(1)).astype(BF)
            values = mm(x, weight(2)).astype(BF).T
            new_tops, new_sums = [], []

            def score(h):
                q = qt_ref[pl.ds(cols + h * head, head), :]
                score_ref[h % DEPTH] = mm(keys[:, h * head : (h + 1) * head], q)

            def soften(h):
                parts = [score_ref[h % DEPTH, j * block : (j + 1) * block, :] for j in range(per_dev)]
                top = tops[h : h + 1, :]
                for j in range(per_dev):
                    peak = jnp.max(parts[j], axis=0, keepdims=True) * scale
                    top = jnp.maximum(top, jnp.where(alive[j], peak, LOW))
                for j in range(per_dev):
                    shift = jnp.where(alive[j], top, -LOW)
                    prob_ref[h % 2, j * block : (j + 1) * block, :] = jnp.exp2(parts[j] * scale - shift).astype(BF)
                new_tops.append(top)

            def mix(h):
                stacked = jnp.concatenate([values[h * head : (h + 1) * head, :], ones], axis=0)
                mixed = mm(stacked, prob_ref[h % 2])
                at = pl.ds(cols + h * head, head)
                if first:
                    new_sums.append(mixed[head : head + 1, :])
                    acc_ref[at, :] = mixed[0:head, :]
                else:
                    fade = jnp.exp2(tops[h : h + 1, :] - new_tops[h])
                    new_sums.append(sums[h : h + 1, :] * fade + mixed[head : head + 1, :])
                    acc_ref[at, :] = acc_in[at, :] * fade + mixed[0:head, :]

            for h in range(DEPTH - 1):
                score(h)
            for h in range(heads_step):
                if h + DEPTH - 1 < heads_step:
                    score(h + DEPTH - 1)
                soften(h)
                if h > 0:
                    mix(h - 1)
            mix(heads_step - 1)
            max_ref[pl.ds(heads_at, heads_step), :] = jnp.concatenate(new_tops, axis=0)
            sum_ref[pl.ds(heads_at, heads_step), :] = jnp.concatenate(new_sums, axis=0)
            return carry

        lax.fori_loop(0, width // GROUP_COLS, group, 0)

    if needed is None:
        run()
    else:
        pl.when(needed)(run)

        @pl.when(jnp.logical_not(needed))
        def _():
            max_ref[...] = max_in[...]
            sum_ref[...] = sum_in[...]
            acc_ref[...] = acc_in[...]

    if last:
        send_ref[0:width, :] = acc_ref[:, rows:queries]
        send_ref[width : width + H, :] = max_ref[:, rows:queries]
        send_ref[width + H : width + 2 * H, :] = sum_ref[:, rows:queries]


def attend_call(mode, step, pieces, state, where, live, w_qkv, rows, block, peers):
    first, last, both = mode
    width = w_qkv.shape[0]
    queries = CORES * rows
    stats = jax.ShapeDtypeStruct((H, queries), F32)
    out_shape = [stats, stats, jax.ShapeDtypeStruct((width, queries), F32)]
    args = [where, live, *pieces, w_qkv]
    aliases = {}
    if first:
        out_shape = [jax.ShapeDtypeStruct((width, queries), BF), *out_shape]
    else:
        args += state
        extra = 1 if last else 0
        aliases = {6: extra, 7: extra + 1, 8: extra + 2}
    if last:
        out_shape = [jax.ShapeDtypeStruct((width + 2 * H, rows), F32), *out_shape]
    out = pl.pallas_call(
        functools.partial(attend_kernel, mode, step, rows, block, peers),
        in_specs=[SMEM, SMEM] + [VMEM] * (len(args) - 2),
        out_specs=[VMEM] * len(out_shape),
        out_shape=out_shape,
        scratch_shapes=[pltpu.VMEM((DEPTH, rows, queries), F32), pltpu.VMEM((2, rows, queries), BF)],
        input_output_aliases=aliases,
        compiler_params=grant(24),
        cost_estimate=pl.CostEstimate(
            flops=4 * rows * width * width + 16 * rows * queries * width,
            transcendentals=H * rows * queries,
            bytes_accessed=4 << 20,
        ),
        name=f"attend{step}{'b' if both else ''}",
    )(*args)
    if first:
        return list(out)
    if last:
        return out
    return [state[0], *out]


def pick_row(tile, at):
    rows = lax.broadcasted_iota(jnp.int32, tile.shape, 0)
    return jnp.sum(jnp.where(rows == at, tile.astype(F32), 0.0), axis=0, keepdims=True)


def add_piece(piece_lists, piece_rows, dests, tile, y_own, y_mate, rows, slot, block):
    numbers = lax.broadcasted_iota(jnp.int32, (rows, slot), 0).astype(F32)
    mixes = []
    for dest in range(CORES):
        chosen = jnp.where(numbers == pick_row(piece_lists, dests[dest]), 1.0, 0.0).astype(BF)
        left = jnp.concatenate([tile(dest, j) for j in range(slot // block)], axis=1)
        mixes.append(mm(left, chosen, ((1,), (1,))).astype(BF))
    both = mm(jnp.concatenate(mixes, axis=0), piece_rows)
    y_own[...] += both[0:rows, :]
    y_mate[...] += both[rows:, :]


def add_arrived(step, where, left_piece, right_piece, spread, y_own, y_mate, rows, slot, block, peers):
    me = where[0]
    mate = me + 1 - 2 * (me % CORES)
    left, right, has_left, has_right = sources_of(step, me, peers)

    def add(source, piece):
        at = rows // block + source * (slot // block)
        add_piece(
            piece[rows:, 0:slot], piece[0:rows, :], (me, mate), lambda dest, j: spread[dest, at + j],
            y_own, y_mate, rows, slot, block,
        )

    pl.when(has_left)(lambda: add(left, left_piece))
    pl.when(has_right)(lambda: add(right, right_piece))


def gather_kernel(steps, far_count, rows, slot, far_slot, block, peers, where, nb_own, nb_mate, *refs):
    own, adj_own, adj_mate, *refs = refs
    arrived = refs[: 2 * steps]
    far = refs[2 * steps : 2 * steps + far_count]
    y_own, y_mate, spread = refs[2 * steps + far_count :]
    me, cluster = where[0], where[1]
    mate = me + 1 - 2 * (me % CORES)
    spread[...] = jnp.zeros(spread.shape, BF)
    per_dev, tiles = adj_own.shape[0], adj_own.shape[1]
    for dest, (adj, nb) in enumerate(((adj_own, nb_own), (adj_mate, nb_mate))):
        for b in range(per_dev):
            for s in range(tiles):
                spread[dest, nb[b, s], b * block : (b + 1) * block, :] = adj[b, s]
    mine = jnp.concatenate([spread[0, j] for j in range(per_dev)], axis=1)
    y_own[...] = mm(mine, own[0:rows, :])
    y_mate[...] = jnp.zeros(y_mate.shape, F32)
    base = rows // block
    add_piece(
        own[rows:, 0:slot], own[0:rows, :], (me, mate),
        lambda dest, j: spread[dest, base + me * (slot // block) + j],
        y_own, y_mate, rows, slot, block,
    )
    first_far = base + peers * (slot // block)
    tiles_far = []
    for f in range(far_count):
        source = far_source(f, cluster, far_count)
        for j in range(far_slot // block):
            tiles_far.append(spread[0, first_far + source * (far_slot // block) + j])
    y_own[...] += mm(jnp.concatenate(tiles_far, axis=1), jnp.concatenate([r[...] for r in far], axis=0))
    for t in range(steps):
        add_arrived(
            t + 1, where, arrived[2 * t], arrived[2 * t + 1], spread, y_own, y_mate, rows, slot, block, peers
        )


def gather_more_kernel(step, rows, slot, block, peers, where, left, right, spread, own_in, mate_in, y_own, y_mate):
    y_own[...] = own_in[...]
    y_mate[...] = mate_in[...]
    add_arrived(step, where, left, right, spread, y_own, y_mate, rows, slot, block, peers)


def far_source(step, cluster, clusters):
    if clusters & (clusters - 1) == 0:
        return cluster ^ step
    return (cluster - step) % clusters


def far_target(step, cluster, clusters):
    if clusters & (clusters - 1) == 0:
        return cluster ^ step
    return (cluster + step) % clusters


def pick_kernel(clusters, where, lists, x, *outs):
    rows = x.shape[0]
    numbers = lax.broadcasted_iota(jnp.int32, (rows, lists.shape[-1]), 0)
    for step, out in enumerate(outs):
        row = lists[0, pl.ds(far_target(step, where[1], clusters), 1), :]
        chosen = jnp.where(numbers == row, 1.0, 0.0).astype(BF)
        out[...] = mm(chosen, x[...], ((0,), (0,))).astype(BF)


def local_kernel(x, y_own, y_got, w, out):
    mixed = (y_own[...] + y_got[...]).astype(BF)
    agg = mm(mixed, w[...])
    out[...] = layer_norm(x[...].astype(F32) + agg)


def tail_kernel(rows, x, local, top, total, acc, got, w_out, w_up, w_down, out):
    heads = top.shape[0]
    width = acc.shape[0]
    head = width // heads
    top_a = top[:, 0:rows]
    top_b = got[width : width + heads, :]
    peak = jnp.maximum(top_a, top_b)
    fade_a = jnp.exp2(top_a - peak)
    fade_b = jnp.exp2(top_b - peak)
    whole = total[:, 0:rows] * fade_a + got[width + heads :, :] * fade_b
    fade_a = fade_a / whole
    fade_b = fade_b / whole
    pieces = []
    for h in range(heads):
        at = slice(h * head, (h + 1) * head)
        pieces.append((acc[at, 0:rows] * fade_a[h : h + 1, :] + got[at, :] * fade_b[h : h + 1, :]).astype(BF))
    attended = jnp.concatenate(pieces, axis=0)
    projected = mm(attended, w_out[...], ((0,), (0,)))
    summed = local[...] + layer_norm(x[...].astype(F32) + projected)
    activated = jax.nn.gelu(mm(summed.astype(BF), w_up[...])).astype(BF)
    out[...] = layer_norm(summed + mm(activated, w_down[...])).astype(BF)


def line_plan(
    node_feats,
    w_gcn,
    adj_tiles,
    neighbor_blocks,
    inner_rows,
    outer_rows,
    w_qkv,
    key_blocks,
    key_counts,
    w_out,
    w_up,
    w_down,
):
    rows, width = node_feats.shape
    block = adj_tiles.shape[-1]
    peers = lax.axis_size("dev")
    clusters = lax.axis_size("group")
    chips = peers // CORES
    slot = inner_rows.shape[-1]
    far_slot = outer_rows.shape[-1]
    cluster = lax.axis_index("group")
    where = jnp.stack([lax.axis_index("dev"), cluster]).astype(jnp.int32)
    swap = [(CORES * c + k, CORES * c + 1 - k) for c in range(chips) for k in range(CORES)]

    def hop(value, step, far):
        pairs = []
        for c in range(chips):
            to = c + step
            if 0 <= to < chips and 0 <= to - step * far < chips:
                pairs += [(CORES * c + k, CORES * to + k) for k in range(CORES)]
        return lax.ppermute(value, "dev", pairs)

    lists = jnp.pad(inner_rows[0].astype(BF), ((0, 0), (0, width - slot)))
    piece = jnp.concatenate([node_feats, lists], axis=0)
    left, right = hop(piece, 1, 1), hop(piece, -1, 1)
    mate_piece = lax.ppermute(piece, "dev", swap)
    mate_adj = lax.ppermute(adj_tiles, "dev", swap)
    mate_nb = lax.ppermute(neighbor_blocks, "dev", swap)

    picked = pl.pallas_call(
        functools.partial(pick_kernel, clusters),
        in_specs=[SMEM, VMEM, VMEM],
        out_specs=[VMEM] * clusters,
        out_shape=[jax.ShapeDtypeStruct((far_slot, width), BF)] * clusters,
        compiler_params=grant(8),
        cost_estimate=pl.CostEstimate(
            flops=2 * rows * clusters * far_slot * width, transcendentals=0, bytes_accessed=1 << 20
        ),
        name="pick",
    )(where, outer_rows, node_feats)
    far = [picked[0]]
    for s in range(1, clusters):
        pairs = [(c, far_target(s, c, clusters)) for c in range(clusters)]
        far.append(lax.ppermute(picked[s], "group", pairs))

    slots = jnp.arange(key_blocks.shape[1], dtype=jnp.int32)[None, :]
    live = jnp.sum(jnp.where(slots < key_counts[:, None], jnp.left_shift(1, key_blocks), 0), axis=1)
    live = live.astype(jnp.int32)

    attend = lambda mode, step, pieces, state: attend_call(
        mode, step, pieces, state, where, live, w_qkv, rows, block, peers
    )
    state = attend((True, False, False), 0, [piece, mate_piece], None)
    arrived = []
    for step in range(1, chips):
        pair = [left, right]
        final = step + 1 == chips
        if final:
            sums = gather_call(
                where, neighbor_blocks, mate_nb, piece, adj_tiles, mate_adj, arrived, far, rows, slot, far_slot, block, peers
            )
            sums = gather_more_call(step, where, pair, sums, rows, slot, block, peers)
            y_got = lax.ppermute(sums[1], "dev", swap)
        else:
            left, right = hop(left, 1, step + 1), hop(right, -1, step + 1)
        two = 2 * step <= chips - 1
        state = attend((False, final and not two, False), step, pair, state)
        if two:
            state = attend((False, final, True), step, pair, state)
        arrived += pair
    send, top, total, acc = state
    got = lax.ppermute(send, "dev", swap)
    local = pl.pallas_call(
        local_kernel,
        in_specs=[VMEM] * 4,
        out_specs=VMEM,
        out_shape=jax.ShapeDtypeStruct((rows, width), F32),
        compiler_params=grant(16),
        cost_estimate=pl.CostEstimate(flops=2 * rows * width * width, transcendentals=0, bytes_accessed=4 << 20),
        name="local",
    )(node_feats, sums[0], y_got, w_gcn)
    return pl.pallas_call(
        functools.partial(tail_kernel, rows),
        in_specs=[VMEM] * 9,
        out_specs=VMEM,
        out_shape=jax.ShapeDtypeStruct((rows, width), BF),
        compiler_params=grant(32),
        cost_estimate=pl.CostEstimate(
            flops=2 * rows * width * (width + 2 * w_up.shape[1]), transcendentals=0, bytes_accessed=12 << 20
        ),
        name="tail",
    )(node_feats, local, top, total, acc, got, w_out, w_up, w_down)


def gather_call(
    where, nb_own, nb_mate, own, adj_own, adj_mate, arrived, far, rows, slot, far_slot, block, peers
):
    width = own.shape[1]
    table_blocks = (rows + peers * slot + len(far) * far_slot) // block
    y = jax.ShapeDtypeStruct((rows, width), F32)
    spread = jax.ShapeDtypeStruct((CORES, table_blocks, rows, block), BF)
    steps = len(arrived) // 2
    return pl.pallas_call(
        functools.partial(gather_kernel, steps, len(far), rows, slot, far_slot, block, peers),
        in_specs=[SMEM] * 3 + [VMEM] * (3 + len(arrived) + len(far)),
        out_specs=[VMEM] * 3,
        out_shape=[y, y, spread],
        compiler_params=grant(24),
        cost_estimate=pl.CostEstimate(
            flops=4 * rows * rows * width * (2 + steps), transcendentals=0, bytes_accessed=8 << 20
        ),
        name="gather",
    )(where, nb_own, nb_mate, own, adj_own, adj_mate, *arrived, *far)


def gather_more_call(step, where, pair, sums, rows, slot, block, peers):
    y_own, y_mate, spread = sums
    return pl.pallas_call(
        functools.partial(gather_more_kernel, step, rows, slot, block, peers),
        in_specs=[SMEM] + [VMEM] * 5,
        out_specs=[VMEM] * 2,
        out_shape=[jax.ShapeDtypeStruct(y_own.shape, F32)] * 2,
        input_output_aliases={4: 0, 5: 1},
        compiler_params=grant(16),
        cost_estimate=pl.CostEstimate(
            flops=4 * rows * rows * y_own.shape[1], transcendentals=0, bytes_accessed=4 << 20
        ),
        name="gather_more",
    )(where, *pair, spread, y_own, y_mate)


def per_device(*args):
    inner, feats, tiles = args[4], args[0], args[2]
    whole_slots = inner.shape[-1] == feats.shape[0] and feats.shape[0] <= 256
    whole_slots = whole_slots and args[8].shape[0] <= 31
    if whole_slots and lax.axis_size("dev") % CORES == 0 and inner.shape[-1] % tiles.shape[-1] == 0:
        return line_plan(*args)
    return gathered_plan(*args)


def solution(mesh):
    placed = (
        P(("group", "dev"), None),
        P(),
        P(("group", "dev"), None, None, None),
        P(("group", "dev"), None),
        P(("group", "dev"), None, None),
        P(("group", "dev"), None, None),
        P(),
        P("group", None),
        P("group"),
        P(),
        P(),
        P(),
    )
    return jax.shard_map(
        per_device, mesh=mesh, in_specs=placed, out_specs=P(("group", "dev"), None), check_vma=False
    )
```

```python
import functools
import math

import jax
import jax.numpy as jnp
from jax import lax
from jax.experimental import pallas as pl
from jax.experimental.pallas import tpu as pltpu
from jax.sharding import PartitionSpec as P


H = 32
LOW = -1e30
CORES = 2


def layer_norm(values):
    average = jnp.mean(values, axis=-1, keepdims=True)
    centered = values - average
    variance = jnp.mean(centered * centered, axis=-1, keepdims=True)
    return centered / jnp.sqrt(variance + 1e-05)


def gathered_plan(
    node_feats,
    w_gcn,
    adj_tiles,
    neighbor_blocks,
    inner_rows,
    outer_rows,
    w_qkv,
    key_blocks,
    key_counts,
    w_out,
    w_up,
    w_down,
):
    row_count = node_feats.shape[0]
    width = node_feats.shape[1]
    block_rows = adj_tiles.shape[-1]
    peers = lax.axis_size("dev")
    clusters = lax.axis_size("group")
    head_size = width // H
    local_heads = H // peers
    head_cols = local_heads * head_size
    gcn_rows = jnp.dot(node_feats, w_gcn, preferred_element_type=jnp.float32).astype(jnp.bfloat16)
    qkv_split = jnp.einsum(
        "rd,dtph->pthr",
        node_feats,
        w_qkv.reshape(width, 3, peers, head_cols),
        preferred_element_type=jnp.float32,
    ).astype(jnp.bfloat16)
    whole_rows, whole_lists = (
        lax.all_gather(gcn_rows, "dev", axis=0, tiled=True),
        lax.all_gather(inner_rows, "dev", axis=0, tiled=True),
    )
    chosen_lists = lax.dynamic_index_in_dim(
        whole_lists, lax.axis_index("dev"), axis=1, keepdims=False
    )
    inner_index = (jnp.arange(peers, dtype=jnp.int32)[:, None] * row_count + chosen_lists).reshape(
        -1
    )
    inner_part = whole_rows[inner_index]
    far_rows, far_lists = (
        lax.all_gather(gcn_rows, "group", axis=0, tiled=True),
        lax.all_gather(outer_rows, "group", axis=0, tiled=True),
    )
    chosen_far = lax.dynamic_index_in_dim(
        far_lists, lax.axis_index("group"), axis=1, keepdims=False
    )
    outer_index = (jnp.arange(clusters, dtype=jnp.int32)[:, None] * row_count + chosen_far).reshape(
        -1
    )
    outer_part = far_rows[outer_index]
    head_parts = lax.all_to_all(qkv_split, "dev", split_axis=0, concat_axis=3, tiled=True)
    table = jnp.concatenate([gcn_rows, inner_part, outer_part], axis=0)
    table_count = table.shape[0] // block_rows
    selector = (
        neighbor_blocks[:, :, None] == jnp.arange(table_count, dtype=jnp.int32)[None, None, :]
    ).astype(jnp.bfloat16)
    spread = jnp.einsum(
        "bst,bsij->bitj", selector, adj_tiles, preferred_element_type=jnp.float32
    ).astype(jnp.bfloat16)
    agg = jnp.dot(
        spread.reshape(row_count, table_count * block_rows),
        table,
        preferred_element_type=jnp.float32,
    )
    features = node_feats.astype(jnp.float32)
    local_branch = layer_norm(features + agg)
    group_rows = row_count * peers
    block_total = group_rows // block_rows
    per_step = 8
    steps_total = block_total // per_step
    head_parts = head_parts.reshape(3, local_heads, head_size, block_total, block_rows)
    query_part = (
        head_parts[0]
        .reshape(local_heads, head_size, steps_total, per_step, block_rows)
        .transpose(2, 0, 1, 3, 4)
    )
    key_value = head_parts[1:3]
    scale = 1.0 / head_size**0.5
    slot_count = key_blocks.shape[1]

    def attend(inputs):
        picks, counts, queries = inputs
        picker = (
            picks[:, :, None] == jnp.arange(block_total, dtype=jnp.int32)[None, None, :]
        ).astype(jnp.bfloat16)
        picked = jnp.einsum(
            "qst,kletj->kleqsj", picker, key_value, preferred_element_type=jnp.float32
        ).astype(jnp.bfloat16)
        keys_here = picked[0]
        values_here = picked[1]
        scores = (
            jnp.einsum("leqi,leqsj->qlisj", queries, keys_here, preferred_element_type=jnp.float32)
            * scale
        )
        live = jnp.arange(slot_count, dtype=jnp.int32)[None, :] < counts[:, None]
        scores = jnp.where(live[:, None, None, :, None], scores, -jnp.inf)
        highest = jnp.max(scores, axis=(3, 4), keepdims=True)
        expos = jnp.exp(scores - highest)
        totals = jnp.sum(expos, axis=(3, 4), keepdims=True)
        probs = (expos / totals).astype(jnp.bfloat16)
        mixed = jnp.einsum(
            "qlisj,leqsj->leqi", probs, values_here, preferred_element_type=jnp.float32
        )
        return mixed.astype(jnp.bfloat16)

    attended = lax.map(
        attend,
        (
            key_blocks.reshape(steps_total, per_step, slot_count),
            key_counts.reshape(steps_total, per_step),
            query_part,
        ),
    )
    attended = attended.transpose(1, 2, 0, 3, 4).reshape(head_cols, group_rows)
    returned = lax.all_to_all(attended, "dev", split_axis=1, concat_axis=0, tiled=True)
    projected = lax.dot_general(
        returned, w_out, (((0,), (0,)), ((), ())), preferred_element_type=jnp.float32
    )
    attn_branch = layer_norm(features + projected)
    summed = local_branch + attn_branch
    summed_in = summed.astype(jnp.bfloat16)
    activated = jax.nn.gelu(jnp.dot(summed_in, w_up, preferred_element_type=jnp.float32)).astype(
        jnp.bfloat16
    )
    layer_out = layer_norm(summed + jnp.dot(activated, w_down, preferred_element_type=jnp.float32))
    return layer_out.astype(jnp.bfloat16)


BF = jnp.bfloat16
F32 = jnp.float32
SMEM = pl.BlockSpec(memory_space=pltpu.SMEM)
VMEM = pl.BlockSpec(memory_space=pltpu.VMEM)
HBM = pl.BlockSpec(memory_space=pltpu.HBM)
GROUP_COLS = 256
DEPTH = 3


def mm(a, b, dims=((1,), (0,))):
    return lax.dot_general(a, b, (dims, ((), ())), preferred_element_type=F32)


def grant(mib):
    return pltpu.CompilerParams(vmem_limit_bytes=mib << 20)


def source_of(step, me, peers):
    chip = me // CORES
    end = (chip == 0) | (chip == peers // CORES - 1)
    if step == 0:
        return me, end
    if step == 1:
        return me ^ CORES, end
    near, across = 2 * CORES, 3 * CORES
    if step == 2:
        return me ^ jnp.where(end, near, across), end
    return me ^ jnp.where(end, across, near), end


def attend_kernel(mode, step, count, rows, block, peers, where, live, *refs):
    first, last = mode
    if first:
        own, mate_piece, w_all, qt_ref, w, max_ref, sum_ref, acc_ref, score_ref, prob_ref, wq_ref, sems = refs
    else:
        arrived, refs = refs[:count], refs[count:]
        qt_ref, w, max_in, sum_in, acc_in, *refs = refs
        if last:
            send_ref, *refs = refs
        max_ref, sum_ref, acc_ref, score_ref, prob_ref = refs
    width = qt_ref.shape[0]
    head = width // H
    heads_step = GROUP_COLS // head
    per_dev = rows // block
    queries = CORES * rows
    scale = math.log2(math.e) / math.sqrt(head)
    me = where[0]
    mate = me + 1 - 2 * (me % CORES)
    source, end = source_of(step, me, peers)

    def loads(g):
        copies = []
        for part in range(3):
            at = part * width + g * GROUP_COLS
            target = wq_ref if part == 0 else w
            to = at if part == 0 else at - width
            copies.append(
                pltpu.make_async_copy(
                    w_all.at[:, pl.ds(pl.multiple_of(at, GROUP_COLS), GROUP_COLS)],
                    target.at[:, pl.ds(pl.multiple_of(to, GROUP_COLS), GROUP_COLS)],
                    sems.at[g, part],
                )
            )
        return copies

    def run():
        if first:
            for g in range(width // GROUP_COLS):
                for load in loads(g):
                    load.start()
            x = own[0:rows, :]
        elif count == 1:
            x = arrived[0][0:rows, :]
        else:
            x = jnp.where(end, arrived[1][0:rows, :], arrived[0][0:rows, :])
        query_blocks = [dev * per_dev + b for dev in (me, mate) for b in range(per_dev)]
        alive = []
        for j in range(per_dev):
            bit = source * per_dev + j
            flags = [jnp.full((1, block), (live[q] >> bit) & 1, jnp.int32) for q in query_blocks]
            alive.append(jnp.concatenate(flags, axis=1) != 0)
        ones = jnp.ones((16, rows), BF)

        def group(g, carry):
            cols = pl.multiple_of(g * GROUP_COLS, GROUP_COLS)
            heads_at = pl.multiple_of(g * heads_step, heads_step)

            def weight(part):
                return w[:, pl.ds(pl.multiple_of(part * width + cols, GROUP_COLS), GROUP_COLS)]

            if first:
                for load in loads(g):
                    load.wait()
                wq = wq_ref[:, pl.ds(cols, GROUP_COLS)]
                qt_ref[pl.ds(cols, GROUP_COLS), 0:rows] = mm(x, wq).astype(BF).T
                mate_q = mm(mate_piece[0:rows, :], wq).astype(BF)
                qt_ref[pl.ds(cols, GROUP_COLS), rows:queries] = mate_q.T
                tops = jnp.full((heads_step, queries), LOW, F32)
                sums = jnp.zeros((heads_step, queries), F32)
            else:
                tops = max_in[pl.ds(heads_at, heads_step), :]
                sums = sum_in[pl.ds(heads_at, heads_step), :]
            keys = mm(x, weight(0)).astype(BF)
            values = mm(x, weight(1)).astype(BF).T
            new_tops, new_sums = [], []

            def score(h):
                q = qt_ref[pl.ds(cols + h * head, head), :]
                score_ref[h % DEPTH] = mm(keys[:, h * head : (h + 1) * head], q)

            def soften(h):
                parts = [score_ref[h % DEPTH, j * block : (j + 1) * block, :] for j in range(per_dev)]
                top = tops[h : h + 1, :]
                for j in range(per_dev):
                    peak = jnp.max(parts[j], axis=0, keepdims=True) * scale
                    top = jnp.maximum(top, jnp.where(alive[j], peak, LOW))
                for j in range(per_dev):
                    shift = jnp.where(alive[j], top, -LOW)
                    prob_ref[h % 2, j * block : (j + 1) * block, :] = jnp.exp2(parts[j] * scale - shift).astype(BF)
                new_tops.append(top)

            def mix(h):
                stacked = jnp.concatenate([values[h * head : (h + 1) * head, :], ones], axis=0)
                mixed = mm(stacked, prob_ref[h % 2])
                at = pl.ds(cols + h * head, head)
                if first:
                    new_sums.append(mixed[head : head + 1, :])
                    acc_ref[at, :] = mixed[0:head, :]
                else:
                    fade = jnp.exp2(tops[h : h + 1, :] - new_tops[h])
                    new_sums.append(sums[h : h + 1, :] * fade + mixed[head : head + 1, :])
                    acc_ref[at, :] = acc_in[at, :] * fade + mixed[0:head, :]

            for h in range(DEPTH - 1):
                score(h)
            for h in range(heads_step):
                if h + DEPTH - 1 < heads_step:
                    score(h + DEPTH - 1)
                soften(h)
                if h > 0:
                    mix(h - 1)
            mix(heads_step - 1)
            max_ref[pl.ds(heads_at, heads_step), :] = jnp.concatenate(new_tops, axis=0)
            sum_ref[pl.ds(heads_at, heads_step), :] = jnp.concatenate(new_sums, axis=0)
            return carry

        lax.fori_loop(0, width // GROUP_COLS, group, 0)

    run()
    if last:
        send_ref[0:width, :] = acc_ref[:, rows:queries]
        send_ref[width : width + H, :] = max_ref[:, rows:queries]
        send_ref[width + H : width + 2 * H, :] = sum_ref[:, rows:queries]


def attend_call(mode, step, pieces, state, where, live, w_qkv, rows, block, peers):
    first, last = mode
    width = w_qkv.shape[0]
    queries = CORES * rows
    stats = jax.ShapeDtypeStruct((H, queries), F32)
    out_shape = [stats, stats, jax.ShapeDtypeStruct((width, queries), F32)]
    scratch = [pltpu.VMEM((DEPTH, rows, queries), F32), pltpu.VMEM((2, rows, queries), BF)]
    args = [where, live, *pieces]
    in_specs = [SMEM] * 2 + [VMEM] * len(pieces)
    aliases = {}
    if first:
        args.append(w_qkv)
        in_specs.append(HBM)
        out_shape = [
            jax.ShapeDtypeStruct((width, queries), BF), jax.ShapeDtypeStruct((width, 2 * width), BF), *out_shape
        ]
        scratch += [pltpu.VMEM((width, width), BF), pltpu.SemaphoreType.DMA((width // GROUP_COLS, 3))]
    else:
        args += state
        in_specs += [VMEM] * len(state)
        extra = 1 if last else 0
        at = len(pieces) + 4
        aliases = {at: extra, at + 1: extra + 1, at + 2: extra + 2}
    if last:
        out_shape = [jax.ShapeDtypeStruct((width + 2 * H, rows), F32), *out_shape]
    out = pl.pallas_call(
        functools.partial(attend_kernel, mode, step, len(pieces), rows, block, peers),
        in_specs=in_specs,
        out_specs=[VMEM] * len(out_shape),
        out_shape=out_shape,
        scratch_shapes=scratch,
        input_output_aliases=aliases,
        compiler_params=grant(42 if first else 24),
        cost_estimate=pl.CostEstimate(
            flops=4 * rows * width * width + 16 * rows * queries * width,
            transcendentals=H * rows * queries,
            bytes_accessed=4 << 20,
        ),
    )(*args)
    if first:
        return list(out)
    if last:
        return out
    return [*state[:2], *out]


def pick_row(tile, at):
    rows = lax.broadcasted_iota(jnp.int32, tile.shape, 0)
    return jnp.sum(jnp.where(rows == at, tile.astype(F32), 0.0), axis=0, keepdims=True)


def add_piece(piece_lists, piece_rows, dests, tile, y_own, y_mate, rows, slot, block):
    numbers = lax.broadcasted_iota(jnp.int32, (rows, slot), 0).astype(F32)
    mixes = []
    for dest in range(CORES):
        chosen = jnp.where(numbers == pick_row(piece_lists, dests[dest]), 1.0, 0.0).astype(BF)
        left = jnp.concatenate([tile(dest, j) for j in range(slot // block)], axis=1)
        mixes.append(mm(left, chosen, ((1,), (1,))).astype(BF))
    both = mm(jnp.concatenate(mixes, axis=0), piece_rows)
    y_own[...] += both[0:rows, :]
    y_mate[...] += both[rows:, :]


def add_arrived(step, where, arrived, spread, y_own, y_mate, rows, slot, block, peers):
    me = where[0]
    mate = me + 1 - 2 * (me % CORES)
    source, end = source_of(step, me, peers)
    at = rows // block + source * (slot // block)
    if len(arrived) == 1:
        lists, x = arrived[0][rows:, 0:slot], arrived[0][0:rows, :]
    else:
        lists = jnp.where(end, arrived[1][rows:, 0:slot], arrived[0][rows:, 0:slot])
        x = jnp.where(end, arrived[1][0:rows, :], arrived[0][0:rows, :])
    add_piece(lists, x, (me, mate), lambda dest, j: spread[dest, at + j], y_own, y_mate, rows, slot, block)


def gather_kernel(steps, far_count, rows, slot, far_slot, block, peers, where, nb_own, nb_mate, *refs):
    own, adj_own, adj_mate, *refs = refs
    count = sum(steps)
    arrived = refs[:count]
    far = refs[count : count + far_count]
    y_own, y_mate, spread = refs[count + far_count :]
    me, cluster = where[0], where[1]
    mate = me + 1 - 2 * (me % CORES)
    spread[...] = jnp.zeros(spread.shape, BF)
    per_dev, tiles = adj_own.shape[0], adj_own.shape[1]
    for dest, (adj, nb) in enumerate(((adj_own, nb_own), (adj_mate, nb_mate))):
        for b in range(per_dev):
            for s in range(tiles):
                spread[dest, nb[b, s], b * block : (b + 1) * block, :] = adj[b, s]
    mine = jnp.concatenate([spread[0, j] for j in range(per_dev)], axis=1)
    y_own[...] = mm(mine, own[0:rows, :])
    y_mate[...] = jnp.zeros(y_mate.shape, F32)
    base = rows // block
    add_piece(
        own[rows:, 0:slot], own[0:rows, :], (me, mate),
        lambda dest, j: spread[dest, base + me * (slot // block) + j],
        y_own, y_mate, rows, slot, block,
    )
    first_far = base + peers * (slot // block)
    tiles_far = []
    for f in range(far_count):
        source = far_source(f, cluster, far_count)
        for j in range(far_slot // block):
            tiles_far.append(spread[0, first_far + source * (far_slot // block) + j])
    y_own[...] += mm(jnp.concatenate(tiles_far, axis=1), jnp.concatenate([r[...] for r in far], axis=0))
    at = 0
    for step, width in enumerate(steps):
        add_arrived(step + 1, where, arrived[at : at + width], spread, y_own, y_mate, rows, slot, block, peers)
        at += width


def gather_more_kernel(step, count, rows, slot, block, peers, where, *refs):
    arrived = refs[:count]
    spread, own_in, mate_in, y_own, y_mate = refs[count:]
    y_own[...] = own_in[...]
    y_mate[...] = mate_in[...]
    add_arrived(step, where, arrived, spread, y_own, y_mate, rows, slot, block, peers)


def far_source(step, cluster, clusters):
    if clusters & (clusters - 1) == 0:
        return cluster ^ step
    return (cluster - step) % clusters


def far_target(step, cluster, clusters):
    if clusters & (clusters - 1) == 0:
        return cluster ^ step
    return (cluster + step) % clusters


def pack_kernel(lists, x, out, sem):
    rows = x.shape[0]
    load = pltpu.make_async_copy(x, out.at[0:rows, :], sem)
    load.start()
    peers, slot = lists.shape[1:]
    numbers = lists[0].astype(F32).astype(BF)
    if slot < out.shape[1]:
        numbers = jnp.concatenate([numbers, jnp.zeros((peers, out.shape[1] - slot), BF)], axis=1)
    out[rows : rows + peers, :] = numbers
    load.wait()


def pick_kernel(clusters, rows, where, lists, x, *outs):
    numbers = lax.broadcasted_iota(jnp.int32, (rows, lists.shape[-1]), 0)
    for step, out in enumerate(outs):
        row = lists[0, pl.ds(far_target(step, where[1], clusters), 1), :]
        chosen = jnp.where(numbers == row, 1.0, 0.0).astype(BF)
        out[...] = mm(chosen, x[0:rows, :], ((0,), (0,))).astype(BF)


def local_kernel(x, y_own, y_got, w, out):
    mixed = (y_own[...] + y_got[...]).astype(BF)
    agg = mm(mixed, w[...])
    out[...] = layer_norm(x[...].astype(F32) + agg)


def tail_kernel(rows, x, local, top, total, acc, got, w_out, w_up_all, w_down, out, w_up, sem):
    load = pltpu.make_async_copy(w_up_all, w_up, sem)
    load.start()
    heads = top.shape[0]
    width = acc.shape[0]
    head = width // heads
    top_a = top[:, 0:rows]
    top_b = got[width : width + heads, :]
    peak = jnp.maximum(top_a, top_b)
    fade_a = jnp.exp2(top_a - peak)
    fade_b = jnp.exp2(top_b - peak)
    whole = total[:, 0:rows] * fade_a + got[width + heads :, :] * fade_b
    fade_a = fade_a / whole
    fade_b = fade_b / whole
    pieces = []
    for h in range(heads):
        at = slice(h * head, (h + 1) * head)
        pieces.append((acc[at, 0:rows] * fade_a[h : h + 1, :] + got[at, :] * fade_b[h : h + 1, :]).astype(BF))
    attended = jnp.concatenate(pieces, axis=0)
    projected = mm(attended, w_out[...], ((0,), (0,)))
    summed = local[...] + layer_norm(x[...].astype(F32) + projected)
    load.wait()
    activated = jax.nn.gelu(mm(summed.astype(BF), w_up[...])).astype(BF)
    out[...] = layer_norm(summed + mm(activated, w_down[...])).astype(BF)


def line_plan(
    node_feats,
    w_gcn,
    adj_tiles,
    neighbor_blocks,
    inner_rows,
    outer_rows,
    w_qkv,
    key_blocks,
    key_counts,
    w_out,
    w_up,
    w_down,
):
    rows, width = node_feats.shape
    block = adj_tiles.shape[-1]
    peers = lax.axis_size("dev")
    clusters = lax.axis_size("group")
    chips = peers // CORES
    slot = inner_rows.shape[-1]
    far_slot = outer_rows.shape[-1]
    cluster = lax.axis_index("group")
    where = jnp.stack([lax.axis_index("dev"), cluster]).astype(jnp.int32)
    swap = [(CORES * c + k, CORES * c + 1 - k) for c in range(chips) for k in range(CORES)]

    def cross(value, pairs):
        lanes = [(CORES * a + k, CORES * b + k) for a, b in pairs for k in range(CORES)]
        return lax.ppermute(value, "dev", lanes)

    piece = pl.pallas_call(
        pack_kernel,
        in_specs=[VMEM, HBM],
        out_specs=VMEM,
        out_shape=jax.ShapeDtypeStruct((rows + peers, width), BF),
        scratch_shapes=[pltpu.SemaphoreType.DMA],
        compiler_params=grant(4),
        name="pack",
    )(inner_rows, node_feats)
    outer, middle = [(0, 1), (1, 0), (2, 3), (3, 2)], [(1, 2), (2, 1)]
    outward = [(1, 0), (2, 3)]
    near, mid = cross(piece, outer), cross(piece, middle)
    mate_piece = lax.ppermute(piece, "dev", swap)
    mate_adj = lax.ppermute(adj_tiles, "dev", swap)
    mate_nb = lax.ppermute(neighbor_blocks, "dev", swap)

    picked = pl.pallas_call(
        functools.partial(pick_kernel, clusters, rows),
        in_specs=[SMEM, VMEM, VMEM],
        out_specs=[VMEM] * clusters,
        out_shape=[jax.ShapeDtypeStruct((far_slot, width), BF)] * clusters,
        compiler_params=grant(8),
        cost_estimate=pl.CostEstimate(
            flops=2 * rows * clusters * far_slot * width, transcendentals=0, bytes_accessed=1 << 20
        ),
        name="pick",
    )(where, outer_rows, piece)
    far = [picked[0]]
    for s in range(1, clusters):
        pairs = [(c, far_target(s, c, clusters)) for c in range(clusters)]
        far.append(lax.ppermute(picked[s], "group", pairs))

    slots = jnp.arange(key_blocks.shape[1], dtype=jnp.int32)[None, :]
    live = jnp.sum(jnp.where(slots < key_counts[:, None], jnp.left_shift(1, key_blocks), 0), axis=1)
    live = live.astype(jnp.int32)

    attend = lambda step, pieces, state, last=False: attend_call(
        (step == 0, last), step, pieces, state, where, live, w_qkv, rows, block, peers
    )
    state = attend(0, [piece, mate_piece], None)
    near, mid, state[2] = lax.optimization_barrier((near, mid, state[2]))
    to_end = cross(mid, outward)
    to_mid = cross(near, middle)
    state = attend(1, [near], state)
    to_mid, to_end, state[2] = lax.optimization_barrier((to_mid, to_end, state[2]))
    across = cross(to_mid, outward)
    state = attend(2, [mid, to_end], state)
    arrived = [near, mid, to_end]
    sums = gather_call(
        where, neighbor_blocks, mate_nb, piece, adj_tiles, mate_adj, arrived, (1, 2), far,
        rows, slot, far_slot, block, peers,
    )
    sums = gather_more_call(3, where, [to_mid, across], sums, rows, slot, block, peers)
    y_send, state[2] = lax.optimization_barrier((sums[1], state[2]))
    y_got = lax.ppermute(y_send, "dev", swap)
    send, top, total, acc = attend(3, [to_mid, across], state, True)
    got = lax.ppermute(send, "dev", swap)
    local = pl.pallas_call(
        local_kernel,
        in_specs=[VMEM] * 4,
        out_specs=VMEM,
        out_shape=jax.ShapeDtypeStruct((rows, width), F32),
        compiler_params=grant(16),
        cost_estimate=pl.CostEstimate(flops=2 * rows * width * width, transcendentals=0, bytes_accessed=4 << 20),
        name="local",
    )(node_feats, sums[0], y_got, w_gcn)
    return pl.pallas_call(
        functools.partial(tail_kernel, rows),
        in_specs=[VMEM] * 7 + [HBM, VMEM],
        out_specs=VMEM,
        out_shape=jax.ShapeDtypeStruct((rows, width), BF),
        scratch_shapes=[pltpu.VMEM(w_up.shape, BF), pltpu.SemaphoreType.DMA],
        compiler_params=grant(32),
        cost_estimate=pl.CostEstimate(
            flops=2 * rows * width * (width + 2 * w_up.shape[1]), transcendentals=0, bytes_accessed=12 << 20
        ),
        name="tail",
    )(node_feats, local, top, total, acc, got, w_out, w_up, w_down)


def gather_call(
    where, nb_own, nb_mate, own, adj_own, adj_mate, arrived, steps, far, rows, slot, far_slot, block, peers
):
    width = own.shape[1]
    table_blocks = (rows + peers * slot + len(far) * far_slot) // block
    y = jax.ShapeDtypeStruct((rows, width), F32)
    spread = jax.ShapeDtypeStruct((CORES, table_blocks, rows, block), BF)
    return pl.pallas_call(
        functools.partial(gather_kernel, steps, len(far), rows, slot, far_slot, block, peers),
        in_specs=[SMEM] * 3 + [VMEM] * (3 + len(arrived) + len(far)),
        out_specs=[VMEM] * 3,
        out_shape=[y, y, spread],
        compiler_params=grant(24),
        cost_estimate=pl.CostEstimate(
            flops=4 * rows * rows * width * (2 + len(steps)), transcendentals=0, bytes_accessed=8 << 20
        ),
        name="gather",
    )(where, nb_own, nb_mate, own, adj_own, adj_mate, *arrived, *far)


def gather_more_call(step, where, pair, sums, rows, slot, block, peers):
    y_own, y_mate, spread = sums
    return pl.pallas_call(
        functools.partial(gather_more_kernel, step, len(pair), rows, slot, block, peers),
        in_specs=[SMEM] + [VMEM] * (len(pair) + 3),
        out_specs=[VMEM] * 2,
        out_shape=[jax.ShapeDtypeStruct(y_own.shape, F32)] * 2,
        input_output_aliases={2 + len(pair): 0, 3 + len(pair): 1},
        compiler_params=grant(16),
        cost_estimate=pl.CostEstimate(
            flops=4 * rows * rows * y_own.shape[1], transcendentals=0, bytes_accessed=4 << 20
        ),
        name="gather_more",
    )(where, *pair, spread, y_own, y_mate)


def per_device(*args):
    inner, feats, tiles = args[4], args[0], args[2]
    whole_slots = inner.shape[-1] == feats.shape[0] and feats.shape[0] <= 256
    whole_slots = whole_slots and args[8].shape[0] <= 31
    if whole_slots and lax.axis_size("dev") == 4 * CORES and inner.shape[-1] % tiles.shape[-1] == 0:
        return line_plan(*args)
    return gathered_plan(*args)


def solution(mesh):
    placed = (
        P(("group", "dev"), None),
        P(),
        P(("group", "dev"), None, None, None),
        P(("group", "dev"), None),
        P(("group", "dev"), None, None),
        P(("group", "dev"), None, None),
        P(),
        P("group", None),
        P("group"),
        P(),
        P(),
        P(),
    )
    return jax.shard_map(per_device, mesh=mesh, in_specs=placed, out_specs=P(("group", "dev"), None), check_vma=False)
```

```python
import functools
import math

import jax
import jax.numpy as jnp
from jax import lax
from jax.experimental import pallas as pl
from jax.experimental.pallas import tpu as pltpu
from jax.sharding import PartitionSpec as P


H = 32
LOW = -1e30
CORES = 2


def layer_norm(values):
    average = jnp.mean(values, axis=-1, keepdims=True)
    centered = values - average
    variance = jnp.mean(centered * centered, axis=-1, keepdims=True)
    return centered / jnp.sqrt(variance + 1e-05)


def gathered_plan(
    node_feats,
    w_gcn,
    adj_tiles,
    neighbor_blocks,
    inner_rows,
    outer_rows,
    w_qkv,
    key_blocks,
    key_counts,
    w_out,
    w_up,
    w_down,
):
    row_count = node_feats.shape[0]
    width = node_feats.shape[1]
    block_rows = adj_tiles.shape[-1]
    peers = lax.axis_size("dev")
    clusters = lax.axis_size("group")
    head_size = width // H
    local_heads = H // peers
    head_cols = local_heads * head_size
    gcn_rows = jnp.dot(node_feats, w_gcn, preferred_element_type=jnp.float32).astype(jnp.bfloat16)
    qkv_split = jnp.einsum(
        "rd,dtph->pthr",
        node_feats,
        w_qkv.reshape(width, 3, peers, head_cols),
        preferred_element_type=jnp.float32,
    ).astype(jnp.bfloat16)
    whole_rows, whole_lists = (
        lax.all_gather(gcn_rows, "dev", axis=0, tiled=True),
        lax.all_gather(inner_rows, "dev", axis=0, tiled=True),
    )
    chosen_lists = lax.dynamic_index_in_dim(
        whole_lists, lax.axis_index("dev"), axis=1, keepdims=False
    )
    inner_index = (jnp.arange(peers, dtype=jnp.int32)[:, None] * row_count + chosen_lists).reshape(
        -1
    )
    inner_part = whole_rows[inner_index]
    far_rows, far_lists = (
        lax.all_gather(gcn_rows, "group", axis=0, tiled=True),
        lax.all_gather(outer_rows, "group", axis=0, tiled=True),
    )
    chosen_far = lax.dynamic_index_in_dim(
        far_lists, lax.axis_index("group"), axis=1, keepdims=False
    )
    outer_index = (jnp.arange(clusters, dtype=jnp.int32)[:, None] * row_count + chosen_far).reshape(
        -1
    )
    outer_part = far_rows[outer_index]
    head_parts = lax.all_to_all(qkv_split, "dev", split_axis=0, concat_axis=3, tiled=True)
    table = jnp.concatenate([gcn_rows, inner_part, outer_part], axis=0)
    table_count = table.shape[0] // block_rows
    selector = (
        neighbor_blocks[:, :, None] == jnp.arange(table_count, dtype=jnp.int32)[None, None, :]
    ).astype(jnp.bfloat16)
    spread = jnp.einsum(
        "bst,bsij->bitj", selector, adj_tiles, preferred_element_type=jnp.float32
    ).astype(jnp.bfloat16)
    agg = jnp.dot(
        spread.reshape(row_count, table_count * block_rows),
        table,
        preferred_element_type=jnp.float32,
    )
    features = node_feats.astype(jnp.float32)
    local_branch = layer_norm(features + agg)
    group_rows = row_count * peers
    block_total = group_rows // block_rows
    per_step = 8
    steps_total = block_total // per_step
    head_parts = head_parts.reshape(3, local_heads, head_size, block_total, block_rows)
    query_part = (
        head_parts[0]
        .reshape(local_heads, head_size, steps_total, per_step, block_rows)
        .transpose(2, 0, 1, 3, 4)
    )
    key_value = head_parts[1:3]
    scale = 1.0 / head_size**0.5
    slot_count = key_blocks.shape[1]

    def attend(inputs):
        picks, counts, queries = inputs
        picker = (
            picks[:, :, None] == jnp.arange(block_total, dtype=jnp.int32)[None, None, :]
        ).astype(jnp.bfloat16)
        picked = jnp.einsum(
            "qst,kletj->kleqsj", picker, key_value, preferred_element_type=jnp.float32
        ).astype(jnp.bfloat16)
        keys_here = picked[0]
        values_here = picked[1]
        scores = (
            jnp.einsum("leqi,leqsj->qlisj", queries, keys_here, preferred_element_type=jnp.float32)
            * scale
        )
        live = jnp.arange(slot_count, dtype=jnp.int32)[None, :] < counts[:, None]
        scores = jnp.where(live[:, None, None, :, None], scores, -jnp.inf)
        highest = jnp.max(scores, axis=(3, 4), keepdims=True)
        expos = jnp.exp(scores - highest)
        totals = jnp.sum(expos, axis=(3, 4), keepdims=True)
        probs = (expos / totals).astype(jnp.bfloat16)
        mixed = jnp.einsum(
            "qlisj,leqsj->leqi", probs, values_here, preferred_element_type=jnp.float32
        )
        return mixed.astype(jnp.bfloat16)

    attended = lax.map(
        attend,
        (
            key_blocks.reshape(steps_total, per_step, slot_count),
            key_counts.reshape(steps_total, per_step),
            query_part,
        ),
    )
    attended = attended.transpose(1, 2, 0, 3, 4).reshape(head_cols, group_rows)
    returned = lax.all_to_all(attended, "dev", split_axis=1, concat_axis=0, tiled=True)
    projected = lax.dot_general(
        returned, w_out, (((0,), (0,)), ((), ())), preferred_element_type=jnp.float32
    )
    attn_branch = layer_norm(features + projected)
    summed = local_branch + attn_branch
    summed_in = summed.astype(jnp.bfloat16)
    activated = jax.nn.gelu(jnp.dot(summed_in, w_up, preferred_element_type=jnp.float32)).astype(
        jnp.bfloat16
    )
    layer_out = layer_norm(summed + jnp.dot(activated, w_down, preferred_element_type=jnp.float32))
    return layer_out.astype(jnp.bfloat16)


BF = jnp.bfloat16
F32 = jnp.float32
SMEM = pl.BlockSpec(memory_space=pltpu.SMEM)
VMEM = pl.BlockSpec(memory_space=pltpu.VMEM)
HBM = pl.BlockSpec(memory_space=pltpu.HBM)
GROUP_COLS = 256
DEPTH = 3


def mm(a, b, dims=((1,), (0,))):
    return lax.dot_general(a, b, (dims, ((), ())), preferred_element_type=F32)


def grant(mib):
    return pltpu.CompilerParams(vmem_limit_bytes=mib << 20)


def source_of(step, me, peers):
    chip = me // CORES
    end = (chip == 0) | (chip == peers // CORES - 1)
    if step == 0:
        return me, end
    return me ^ (CORES * (1, 3, 2)[step - 1]), end


def attend_kernel(mode, step, count, rows, block, peers, where, live, *refs):
    first, last = mode
    if first:
        own, mate_piece, w_all, qt_ref, w, max_ref, sum_ref, acc_ref, score_ref, prob_ref, wq_ref, sems = refs
    else:
        arrived, refs = refs[:count], refs[count:]
        qt_ref, w, max_in, sum_in, acc_in, *refs = refs
        if last:
            send_ref, *refs = refs
        max_ref, sum_ref, acc_ref, score_ref, prob_ref = refs
    width = qt_ref.shape[0]
    head = width // H
    heads_step = GROUP_COLS // head
    per_dev = rows // block
    queries = CORES * rows
    scale = math.log2(math.e) / math.sqrt(head)
    me = where[0]
    mate = me + 1 - 2 * (me % CORES)
    source, end = source_of(step, me, peers)

    def loads(g):
        copies = []
        for part in range(3):
            at = part * width + g * GROUP_COLS
            target = wq_ref if part == 0 else w
            to = at if part == 0 else at - width
            copies.append(
                pltpu.make_async_copy(
                    w_all.at[:, pl.ds(pl.multiple_of(at, GROUP_COLS), GROUP_COLS)],
                    target.at[:, pl.ds(pl.multiple_of(to, GROUP_COLS), GROUP_COLS)],
                    sems.at[g, part],
                )
            )
        return copies

    def run():
        if first:
            for g in range(width // GROUP_COLS):
                for load in loads(g):
                    load.start()
            x = own[0:rows, :]
        elif count == 1:
            x = arrived[0][0:rows, :]
        else:
            x = jnp.where(end, arrived[1][0:rows, :], arrived[0][0:rows, :])
        query_blocks = [dev * per_dev + b for dev in (me, mate) for b in range(per_dev)]
        alive = []
        for j in range(per_dev):
            bit = source * per_dev + j
            flags = [jnp.full((1, block), (live[q] >> bit) & 1, jnp.int32) for q in query_blocks]
            alive.append(jnp.concatenate(flags, axis=1) != 0)
        ones = jnp.ones((16, rows), BF)

        def group(g, carry):
            cols = pl.multiple_of(g * GROUP_COLS, GROUP_COLS)
            heads_at = pl.multiple_of(g * heads_step, heads_step)

            def weight(part):
                return w[:, pl.ds(pl.multiple_of(part * width + cols, GROUP_COLS), GROUP_COLS)]

            if first:
                for load in loads(g):
                    load.wait()
                wq = wq_ref[:, pl.ds(cols, GROUP_COLS)]
                qt_ref[pl.ds(cols, GROUP_COLS), 0:rows] = mm(x, wq).astype(BF).T
                mate_q = mm(mate_piece[0:rows, :], wq).astype(BF)
                qt_ref[pl.ds(cols, GROUP_COLS), rows:queries] = mate_q.T
                tops = jnp.full((heads_step, queries), LOW, F32)
                sums = jnp.zeros((heads_step, queries), F32)
            else:
                tops = max_in[pl.ds(heads_at, heads_step), :]
                sums = sum_in[pl.ds(heads_at, heads_step), :]
            keys = mm(x, weight(0)).astype(BF)
            values = mm(x, weight(1)).astype(BF).T
            new_tops, new_sums = [], []

            def score(h):
                q = qt_ref[pl.ds(cols + h * head, head), :]
                score_ref[h % DEPTH] = mm(keys[:, h * head : (h + 1) * head], q)

            def soften(h):
                parts = [score_ref[h % DEPTH, j * block : (j + 1) * block, :] for j in range(per_dev)]
                top = tops[h : h + 1, :]
                for j in range(per_dev):
                    peak = jnp.max(parts[j], axis=0, keepdims=True) * scale
                    top = jnp.maximum(top, jnp.where(alive[j], peak, LOW))
                for j in range(per_dev):
                    shift = jnp.where(alive[j], top, -LOW)
                    prob_ref[h % 2, j * block : (j + 1) * block, :] = jnp.exp2(parts[j] * scale - shift).astype(BF)
                new_tops.append(top)

            def mix(h):
                stacked = jnp.concatenate([values[h * head : (h + 1) * head, :], ones], axis=0)
                mixed = mm(stacked, prob_ref[h % 2])
                at = pl.ds(cols + h * head, head)
                if first:
                    new_sums.append(mixed[head : head + 1, :])
                    acc_ref[at, :] = mixed[0:head, :]
                else:
                    fade = jnp.exp2(tops[h : h + 1, :] - new_tops[h])
                    new_sums.append(sums[h : h + 1, :] * fade + mixed[head : head + 1, :])
                    acc_ref[at, :] = acc_in[at, :] * fade + mixed[0:head, :]

            for h in range(DEPTH - 1):
                score(h)
            for h in range(heads_step):
                if h + DEPTH - 1 < heads_step:
                    score(h + DEPTH - 1)
                soften(h)
                if h > 0:
                    mix(h - 1)
            mix(heads_step - 1)
            max_ref[pl.ds(heads_at, heads_step), :] = jnp.concatenate(new_tops, axis=0)
            sum_ref[pl.ds(heads_at, heads_step), :] = jnp.concatenate(new_sums, axis=0)
            return carry

        lax.fori_loop(0, width // GROUP_COLS, group, 0)

    run()
    if last:
        send_ref[0:width, :] = acc_ref[:, rows:queries]
        send_ref[width : width + H, :] = max_ref[:, rows:queries]
        send_ref[width + H : width + 2 * H, :] = sum_ref[:, rows:queries]


def attend_call(mode, step, pieces, state, where, live, w_qkv, rows, block, peers):
    first, last = mode
    width = w_qkv.shape[0]
    queries = CORES * rows
    stats = jax.ShapeDtypeStruct((H, queries), F32)
    out_shape = [stats, stats, jax.ShapeDtypeStruct((width, queries), F32)]
    scratch = [pltpu.VMEM((DEPTH, rows, queries), F32), pltpu.VMEM((2, rows, queries), BF)]
    args = [where, live, *pieces]
    in_specs = [SMEM] * 2 + [VMEM] * len(pieces)
    aliases = {}
    if first:
        args.append(w_qkv)
        in_specs.append(HBM)
        out_shape = [
            jax.ShapeDtypeStruct((width, queries), BF), jax.ShapeDtypeStruct((width, 2 * width), BF), *out_shape
        ]
        scratch += [pltpu.VMEM((width, width), BF), pltpu.SemaphoreType.DMA((width // GROUP_COLS, 3))]
    else:
        args += state
        in_specs += [VMEM] * len(state)
        extra = 1 if last else 0
        at = len(pieces) + 4
        aliases = {at: extra, at + 1: extra + 1, at + 2: extra + 2}
    if last:
        out_shape = [jax.ShapeDtypeStruct((width + 2 * H, rows), F32), *out_shape]
    out = pl.pallas_call(
        functools.partial(attend_kernel, mode, step, len(pieces), rows, block, peers),
        in_specs=in_specs,
        out_specs=[VMEM] * len(out_shape),
        out_shape=out_shape,
        scratch_shapes=scratch,
        input_output_aliases=aliases,
        compiler_params=grant(42 if first else 24),
        cost_estimate=pl.CostEstimate(
            flops=4 * rows * width * width + 16 * rows * queries * width,
            transcendentals=H * rows * queries,
            bytes_accessed=4 << 20,
        ),
    )(*args)
    if first:
        return list(out)
    if last:
        return out
    return [*state[:2], *out]


def pick_row(tile, at):
    rows = lax.broadcasted_iota(jnp.int32, tile.shape, 0)
    return jnp.sum(jnp.where(rows == at, tile.astype(F32), 0.0), axis=0, keepdims=True)


def add_piece(piece_lists, piece_rows, dests, tile, y_own, y_mate, rows, slot, block):
    numbers = lax.broadcasted_iota(jnp.int32, (rows, slot), 0).astype(F32)
    mixes = []
    for dest in range(CORES):
        chosen = jnp.where(numbers == pick_row(piece_lists, dests[dest]), 1.0, 0.0).astype(BF)
        left = jnp.concatenate([tile(dest, j) for j in range(slot // block)], axis=1)
        mixes.append(mm(left, chosen, ((1,), (1,))).astype(BF))
    both = mm(jnp.concatenate(mixes, axis=0), piece_rows)
    y_own[...] += both[0:rows, :]
    y_mate[...] += both[rows:, :]


def add_arrived(step, where, arrived, spread, y_own, y_mate, rows, slot, block, peers):
    me = where[0]
    mate = me + 1 - 2 * (me % CORES)
    source, end = source_of(step, me, peers)
    at = rows // block + source * (slot // block)
    if len(arrived) == 1:
        lists, x = arrived[0][rows:, 0:slot], arrived[0][0:rows, :]
    else:
        lists = jnp.where(end, arrived[1][rows:, 0:slot], arrived[0][rows:, 0:slot])
        x = jnp.where(end, arrived[1][0:rows, :], arrived[0][0:rows, :])
    add_piece(lists, x, (me, mate), lambda dest, j: spread[dest, at + j], y_own, y_mate, rows, slot, block)


def gather_kernel(steps, far_count, rows, slot, far_slot, block, peers, where, nb_own, nb_mate, *refs):
    own, adj_own, adj_mate, *refs = refs
    count = sum(steps)
    arrived = refs[:count]
    far = refs[count : count + far_count]
    y_own, y_mate, spread = refs[count + far_count :]
    me, cluster = where[0], where[1]
    mate = me + 1 - 2 * (me % CORES)
    spread[...] = jnp.zeros(spread.shape, BF)
    per_dev, tiles = adj_own.shape[0], adj_own.shape[1]
    for dest, (adj, nb) in enumerate(((adj_own, nb_own), (adj_mate, nb_mate))):
        for b in range(per_dev):
            for s in range(tiles):
                spread[dest, nb[b, s], b * block : (b + 1) * block, :] = adj[b, s]
    mine = jnp.concatenate([spread[0, j] for j in range(per_dev)], axis=1)
    y_own[...] = mm(mine, own[0:rows, :])
    y_mate[...] = jnp.zeros(y_mate.shape, F32)
    base = rows // block
    add_piece(
        own[rows:, 0:slot], own[0:rows, :], (me, mate),
        lambda dest, j: spread[dest, base + me * (slot // block) + j],
        y_own, y_mate, rows, slot, block,
    )
    first_far = base + peers * (slot // block)
    tiles_far = []
    for f in range(far_count):
        source = far_source(f, cluster, far_count)
        for j in range(far_slot // block):
            tiles_far.append(spread[0, first_far + source * (far_slot // block) + j])
    y_own[...] += mm(jnp.concatenate(tiles_far, axis=1), jnp.concatenate([r[...] for r in far], axis=0))
    at = 0
    for step, width in enumerate(steps):
        add_arrived(step + 1, where, arrived[at : at + width], spread, y_own, y_mate, rows, slot, block, peers)
        at += width


def gather_more_kernel(step, count, rows, slot, block, peers, where, *refs):
    arrived = refs[:count]
    spread, own_in, mate_in, y_own, y_mate = refs[count:]
    y_own[...] = own_in[...]
    y_mate[...] = mate_in[...]
    add_arrived(step, where, arrived, spread, y_own, y_mate, rows, slot, block, peers)


def far_source(step, cluster, clusters):
    if clusters & (clusters - 1) == 0:
        return cluster ^ step
    return (cluster - step) % clusters


def far_target(step, cluster, clusters):
    if clusters & (clusters - 1) == 0:
        return cluster ^ step
    return (cluster + step) % clusters


def pack_kernel(lists, x, out, sem):
    rows = x.shape[0]
    load = pltpu.make_async_copy(x, out.at[0:rows, :], sem)
    load.start()
    peers, slot = lists.shape[1:]
    numbers = lists[0].astype(F32).astype(BF)
    if slot < out.shape[1]:
        numbers = jnp.concatenate([numbers, jnp.zeros((peers, out.shape[1] - slot), BF)], axis=1)
    out[rows : rows + peers, :] = numbers
    load.wait()


def pick_kernel(clusters, rows, where, lists, x, *outs):
    numbers = lax.broadcasted_iota(jnp.int32, (rows, lists.shape[-1]), 0)
    for step, out in enumerate(outs):
        row = lists[0, pl.ds(far_target(step, where[1], clusters), 1), :]
        chosen = jnp.where(numbers == row, 1.0, 0.0).astype(BF)
        out[...] = mm(chosen, x[0:rows, :], ((0,), (0,))).astype(BF)


def local_kernel(x, y_own, y_got, w, out):
    mixed = (y_own[...] + y_got[...]).astype(BF)
    agg = mm(mixed, w[...])
    out[...] = layer_norm(x[...].astype(F32) + agg)


def tail_kernel(rows, x, local, top, total, acc, got, w_out, w_up_all, w_down, out, w_up, sem):
    load = pltpu.make_async_copy(w_up_all, w_up, sem)
    load.start()
    heads = top.shape[0]
    width = acc.shape[0]
    head = width // heads
    top_a = top[:, 0:rows]
    top_b = got[width : width + heads, :]
    peak = jnp.maximum(top_a, top_b)
    fade_a = jnp.exp2(top_a - peak)
    fade_b = jnp.exp2(top_b - peak)
    whole = total[:, 0:rows] * fade_a + got[width + heads :, :] * fade_b
    fade_a = fade_a / whole
    fade_b = fade_b / whole
    pieces = []
    for h in range(heads):
        at = slice(h * head, (h + 1) * head)
        pieces.append((acc[at, 0:rows] * fade_a[h : h + 1, :] + got[at, :] * fade_b[h : h + 1, :]).astype(BF))
    attended = jnp.concatenate(pieces, axis=0)
    projected = mm(attended, w_out[...], ((0,), (0,)))
    summed = local[...] + layer_norm(x[...].astype(F32) + projected)
    load.wait()
    activated = jax.nn.gelu(mm(summed.astype(BF), w_up[...])).astype(BF)
    out[...] = layer_norm(summed + mm(activated, w_down[...])).astype(BF)


def line_plan(
    node_feats,
    w_gcn,
    adj_tiles,
    neighbor_blocks,
    inner_rows,
    outer_rows,
    w_qkv,
    key_blocks,
    key_counts,
    w_out,
    w_up,
    w_down,
):
    rows, width = node_feats.shape
    block = adj_tiles.shape[-1]
    peers = lax.axis_size("dev")
    clusters = lax.axis_size("group")
    chips = peers // CORES
    slot = inner_rows.shape[-1]
    far_slot = outer_rows.shape[-1]
    cluster = lax.axis_index("group")
    where = jnp.stack([lax.axis_index("dev"), cluster]).astype(jnp.int32)
    swap = [(CORES * c + k, CORES * c + 1 - k) for c in range(chips) for k in range(CORES)]

    def cross(value, pairs):
        lanes = [(CORES * a + k, CORES * b + k) for a, b in pairs for k in range(CORES)]
        return lax.ppermute(value, "dev", lanes)

    piece = pl.pallas_call(
        pack_kernel,
        in_specs=[VMEM, HBM],
        out_specs=VMEM,
        out_shape=jax.ShapeDtypeStruct((rows + peers, width), BF),
        scratch_shapes=[pltpu.SemaphoreType.DMA],
        compiler_params=grant(4),
        name="pack",
    )(inner_rows, node_feats)
    outer, middle = [(0, 1), (1, 0), (2, 3), (3, 2)], [(1, 2), (2, 1)]
    outward = [(1, 0), (2, 3)]
    near, mid = cross(piece, outer), cross(piece, middle)
    mate_piece = lax.ppermute(piece, "dev", swap)
    mate_adj = lax.ppermute(adj_tiles, "dev", swap)
    mate_nb = lax.ppermute(neighbor_blocks, "dev", swap)

    picked = pl.pallas_call(
        functools.partial(pick_kernel, clusters, rows),
        in_specs=[SMEM, VMEM, VMEM],
        out_specs=[VMEM] * clusters,
        out_shape=[jax.ShapeDtypeStruct((far_slot, width), BF)] * clusters,
        compiler_params=grant(8),
        cost_estimate=pl.CostEstimate(
            flops=2 * rows * clusters * far_slot * width, transcendentals=0, bytes_accessed=1 << 20
        ),
        name="pick",
    )(where, outer_rows, piece)
    far = [picked[0]]
    for s in range(1, clusters):
        pairs = [(c, far_target(s, c, clusters)) for c in range(clusters)]
        far.append(lax.ppermute(picked[s], "group", pairs))

    slots = jnp.arange(key_blocks.shape[1], dtype=jnp.int32)[None, :]
    live = jnp.sum(jnp.where(slots < key_counts[:, None], jnp.left_shift(1, key_blocks), 0), axis=1)
    live = live.astype(jnp.int32)

    attend = lambda step, pieces, state, last=False: attend_call(
        (step == 0, last), step, pieces, state, where, live, w_qkv, rows, block, peers
    )
    state = attend(0, [piece, mate_piece], None)
    near, mid, to_far, state[2] = lax.optimization_barrier((near, mid, piece, state[2]))
    ends = cross(to_far, [(0, 3), (3, 0)])
    to_end = cross(mid, outward)
    to_mid = cross(near, middle)
    state = attend(1, [near], state)
    state = attend(2, [mid, ends], state)
    sums = gather_call(
        where, neighbor_blocks, mate_nb, piece, adj_tiles, mate_adj, [near, mid, ends], (1, 2), far,
        rows, slot, far_slot, block, peers,
    )
    sums = gather_more_call(3, where, [to_mid, to_end], sums, rows, slot, block, peers)
    y_send, state[2] = lax.optimization_barrier((sums[1], state[2]))
    y_got = lax.ppermute(y_send, "dev", swap)
    send, top, total, acc = attend(3, [to_mid, to_end], state, True)
    got = lax.ppermute(send, "dev", swap)
    local = pl.pallas_call(
        local_kernel,
        in_specs=[VMEM] * 4,
        out_specs=VMEM,
        out_shape=jax.ShapeDtypeStruct((rows, width), F32),
        compiler_params=grant(16),
        cost_estimate=pl.CostEstimate(flops=2 * rows * width * width, transcendentals=0, bytes_accessed=4 << 20),
        name="local",
    )(node_feats, sums[0], y_got, w_gcn)
    return pl.pallas_call(
        functools.partial(tail_kernel, rows),
        in_specs=[VMEM] * 7 + [HBM, VMEM],
        out_specs=VMEM,
        out_shape=jax.ShapeDtypeStruct((rows, width), BF),
        scratch_shapes=[pltpu.VMEM(w_up.shape, BF), pltpu.SemaphoreType.DMA],
        compiler_params=grant(32),
        cost_estimate=pl.CostEstimate(
            flops=2 * rows * width * (width + 2 * w_up.shape[1]), transcendentals=0, bytes_accessed=12 << 20
        ),
        name="tail",
    )(node_feats, local, top, total, acc, got, w_out, w_up, w_down)


def gather_call(
    where, nb_own, nb_mate, own, adj_own, adj_mate, arrived, steps, far, rows, slot, far_slot, block, peers
):
    width = own.shape[1]
    table_blocks = (rows + peers * slot + len(far) * far_slot) // block
    y = jax.ShapeDtypeStruct((rows, width), F32)
    spread = jax.ShapeDtypeStruct((CORES, table_blocks, rows, block), BF)
    return pl.pallas_call(
        functools.partial(gather_kernel, steps, len(far), rows, slot, far_slot, block, peers),
        in_specs=[SMEM] * 3 + [VMEM] * (3 + len(arrived) + len(far)),
        out_specs=[VMEM] * 3,
        out_shape=[y, y, spread],
        compiler_params=grant(24),
        cost_estimate=pl.CostEstimate(
            flops=4 * rows * rows * width * (2 + len(steps)), transcendentals=0, bytes_accessed=8 << 20
        ),
        name="gather",
    )(where, nb_own, nb_mate, own, adj_own, adj_mate, *arrived, *far)


def gather_more_call(step, where, pair, sums, rows, slot, block, peers):
    y_own, y_mate, spread = sums
    return pl.pallas_call(
        functools.partial(gather_more_kernel, step, len(pair), rows, slot, block, peers),
        in_specs=[SMEM] + [VMEM] * (len(pair) + 3),
        out_specs=[VMEM] * 2,
        out_shape=[jax.ShapeDtypeStruct(y_own.shape, F32)] * 2,
        input_output_aliases={2 + len(pair): 0, 3 + len(pair): 1},
        compiler_params=grant(16),
        cost_estimate=pl.CostEstimate(
            flops=4 * rows * rows * y_own.shape[1], transcendentals=0, bytes_accessed=4 << 20
        ),
        name="gather_more",
    )(where, *pair, spread, y_own, y_mate)


def per_device(*args):
    inner, feats, tiles = args[4], args[0], args[2]
    whole_slots = inner.shape[-1] == feats.shape[0] and feats.shape[0] <= 256
    whole_slots = whole_slots and args[8].shape[0] <= 31
    if whole_slots and lax.axis_size("dev") == 4 * CORES and inner.shape[-1] % tiles.shape[-1] == 0:
        return line_plan(*args)
    return gathered_plan(*args)


def solution(mesh):
    placed = (
        P(("group", "dev"), None),
        P(),
        P(("group", "dev"), None, None, None),
        P(("group", "dev"), None),
        P(("group", "dev"), None, None),
        P(("group", "dev"), None, None),
        P(),
        P("group", None),
        P("group"),
        P(),
        P(),
        P(),
    )
    return jax.shard_map(per_device, mesh=mesh, in_specs=placed, out_specs=P(("group", "dev"), None), check_vma=False)
```

```python
import functools
import math

import jax
import jax.numpy as jnp
from jax import lax
from jax.experimental import pallas as pl
from jax.experimental.pallas import tpu as pltpu
from jax.sharding import PartitionSpec as P


H = 32
LOW = -1e30
CORES = 2


def layer_norm(values):
    average = jnp.mean(values, axis=-1, keepdims=True)
    centered = values - average
    variance = jnp.mean(centered * centered, axis=-1, keepdims=True)
    return centered / jnp.sqrt(variance + 1e-05)


def gathered_plan(
    node_feats,
    w_gcn,
    adj_tiles,
    neighbor_blocks,
    inner_rows,
    outer_rows,
    w_qkv,
    key_blocks,
    key_counts,
    w_out,
    w_up,
    w_down,
):
    row_count = node_feats.shape[0]
    width = node_feats.shape[1]
    block_rows = adj_tiles.shape[-1]
    peers = lax.axis_size("dev")
    clusters = lax.axis_size("group")
    head_size = width // H
    local_heads = H // peers
    head_cols = local_heads * head_size
    gcn_rows = jnp.dot(node_feats, w_gcn, preferred_element_type=jnp.float32).astype(jnp.bfloat16)
    qkv_split = jnp.einsum(
        "rd,dtph->pthr",
        node_feats,
        w_qkv.reshape(width, 3, peers, head_cols),
        preferred_element_type=jnp.float32,
    ).astype(jnp.bfloat16)
    whole_rows, whole_lists = (
        lax.all_gather(gcn_rows, "dev", axis=0, tiled=True),
        lax.all_gather(inner_rows, "dev", axis=0, tiled=True),
    )
    chosen_lists = lax.dynamic_index_in_dim(
        whole_lists, lax.axis_index("dev"), axis=1, keepdims=False
    )
    inner_index = (jnp.arange(peers, dtype=jnp.int32)[:, None] * row_count + chosen_lists).reshape(
        -1
    )
    inner_part = whole_rows[inner_index]
    far_rows, far_lists = (
        lax.all_gather(gcn_rows, "group", axis=0, tiled=True),
        lax.all_gather(outer_rows, "group", axis=0, tiled=True),
    )
    chosen_far = lax.dynamic_index_in_dim(
        far_lists, lax.axis_index("group"), axis=1, keepdims=False
    )
    outer_index = (jnp.arange(clusters, dtype=jnp.int32)[:, None] * row_count + chosen_far).reshape(
        -1
    )
    outer_part = far_rows[outer_index]
    head_parts = lax.all_to_all(qkv_split, "dev", split_axis=0, concat_axis=3, tiled=True)
    table = jnp.concatenate([gcn_rows, inner_part, outer_part], axis=0)
    table_count = table.shape[0] // block_rows
    selector = (
        neighbor_blocks[:, :, None] == jnp.arange(table_count, dtype=jnp.int32)[None, None, :]
    ).astype(jnp.bfloat16)
    spread = jnp.einsum(
        "bst,bsij->bitj", selector, adj_tiles, preferred_element_type=jnp.float32
    ).astype(jnp.bfloat16)
    agg = jnp.dot(
        spread.reshape(row_count, table_count * block_rows),
        table,
        preferred_element_type=jnp.float32,
    )
    features = node_feats.astype(jnp.float32)
    local_branch = layer_norm(features + agg)
    group_rows = row_count * peers
    block_total = group_rows // block_rows
    per_step = 8
    steps_total = block_total // per_step
    head_parts = head_parts.reshape(3, local_heads, head_size, block_total, block_rows)
    query_part = (
        head_parts[0]
        .reshape(local_heads, head_size, steps_total, per_step, block_rows)
        .transpose(2, 0, 1, 3, 4)
    )
    key_value = head_parts[1:3]
    scale = 1.0 / head_size**0.5
    slot_count = key_blocks.shape[1]

    def attend(inputs):
        picks, counts, queries = inputs
        picker = (
            picks[:, :, None] == jnp.arange(block_total, dtype=jnp.int32)[None, None, :]
        ).astype(jnp.bfloat16)
        picked = jnp.einsum(
            "qst,kletj->kleqsj", picker, key_value, preferred_element_type=jnp.float32
        ).astype(jnp.bfloat16)
        keys_here = picked[0]
        values_here = picked[1]
        scores = (
            jnp.einsum("leqi,leqsj->qlisj", queries, keys_here, preferred_element_type=jnp.float32)
            * scale
        )
        live = jnp.arange(slot_count, dtype=jnp.int32)[None, :] < counts[:, None]
        scores = jnp.where(live[:, None, None, :, None], scores, -jnp.inf)
        highest = jnp.max(scores, axis=(3, 4), keepdims=True)
        expos = jnp.exp(scores - highest)
        totals = jnp.sum(expos, axis=(3, 4), keepdims=True)
        probs = (expos / totals).astype(jnp.bfloat16)
        mixed = jnp.einsum(
            "qlisj,leqsj->leqi", probs, values_here, preferred_element_type=jnp.float32
        )
        return mixed.astype(jnp.bfloat16)

    attended = lax.map(
        attend,
        (
            key_blocks.reshape(steps_total, per_step, slot_count),
            key_counts.reshape(steps_total, per_step),
            query_part,
        ),
    )
    attended = attended.transpose(1, 2, 0, 3, 4).reshape(head_cols, group_rows)
    returned = lax.all_to_all(attended, "dev", split_axis=1, concat_axis=0, tiled=True)
    projected = lax.dot_general(
        returned, w_out, (((0,), (0,)), ((), ())), preferred_element_type=jnp.float32
    )
    attn_branch = layer_norm(features + projected)
    summed = local_branch + attn_branch
    summed_in = summed.astype(jnp.bfloat16)
    activated = jax.nn.gelu(jnp.dot(summed_in, w_up, preferred_element_type=jnp.float32)).astype(
        jnp.bfloat16
    )
    layer_out = layer_norm(summed + jnp.dot(activated, w_down, preferred_element_type=jnp.float32))
    return layer_out.astype(jnp.bfloat16)


BF = jnp.bfloat16
F32 = jnp.float32
SMEM = pl.BlockSpec(memory_space=pltpu.SMEM)
VMEM = pl.BlockSpec(memory_space=pltpu.VMEM)
HBM = pl.BlockSpec(memory_space=pltpu.HBM)
GROUP_COLS = 256
DEPTH = 3


def mm(a, b, dims=((1,), (0,))):
    return lax.dot_general(a, b, (dims, ((), ())), preferred_element_type=F32)


def grant(mib):
    return pltpu.CompilerParams(vmem_limit_bytes=mib << 20)


def source_of(step, me, peers):
    chip = me // CORES
    end = (chip == 0) | (chip == peers // CORES - 1)
    if step == 0:
        return me, end
    return me ^ (CORES * (1, 3, 2)[step - 1]), end


def attend_kernel(mode, step, count, rows, block, peers, where, live, *refs):
    first, last = mode
    if first:
        own, mate_piece, w_all, qt_ref, w, max_ref, sum_ref, acc_ref, score_ref, prob_ref, key_ref, value_ref, wq_ref, sems = refs
    else:
        arrived, refs = refs[:count], refs[count:]
        qt_ref, w, max_in, sum_in, acc_in, *refs = refs
        if last:
            send_ref, *refs = refs
        max_ref, sum_ref, acc_ref, score_ref, prob_ref, key_ref, value_ref = refs
    width = qt_ref.shape[0]
    head = width // H
    heads_step = GROUP_COLS // head
    per_dev = rows // block
    queries = CORES * rows
    scale = math.log2(math.e) / math.sqrt(head)
    me = where[0]
    mate = me + 1 - 2 * (me % CORES)
    source, end = source_of(step, me, peers)

    def loads(g):
        copies = []
        for part in range(3):
            at = part * width + g * GROUP_COLS
            target = wq_ref if part == 0 else w
            to = at if part == 0 else at - width
            copies.append(
                pltpu.make_async_copy(
                    w_all.at[:, pl.ds(pl.multiple_of(at, GROUP_COLS), GROUP_COLS)],
                    target.at[:, pl.ds(pl.multiple_of(to, GROUP_COLS), GROUP_COLS)],
                    sems.at[g, part],
                )
            )
        return copies

    def run():
        if first:
            for g in range(width // GROUP_COLS):
                for load in loads(g):
                    load.start()
            x = own[0:rows, :]
        elif count == 1:
            x = arrived[0][0:rows, :]
        else:
            x = jnp.where(end, arrived[1][0:rows, :], arrived[0][0:rows, :])
        query_blocks = [dev * per_dev + b for dev in (me, mate) for b in range(per_dev)]
        alive = []
        for j in range(per_dev):
            bit = source * per_dev + j
            flags = [jnp.full((1, block), (live[q] >> bit) & 1, jnp.int32) for q in query_blocks]
            alive.append(jnp.concatenate(flags, axis=1) != 0)
        ones = jnp.ones((16, rows), BF)

        def columns(g):
            return pl.multiple_of(g * GROUP_COLS, GROUP_COLS)

        def project(g, slot):
            cols = columns(g)
            if first:
                wq = wq_ref[:, pl.ds(cols, GROUP_COLS)]
                qt_ref[pl.ds(cols, GROUP_COLS), 0:rows] = (mm(x, wq) * scale).astype(BF).T
                mate_q = (mm(mate_piece[0:rows, :], wq) * scale).astype(BF)
                qt_ref[pl.ds(cols, GROUP_COLS), rows:queries] = mate_q.T
            key_ref[slot] = mm(x, w[:, pl.ds(cols, GROUP_COLS)]).astype(BF)
            values = mm(x, w[:, pl.ds(columns(g) + width, GROUP_COLS)]).astype(BF)
            value_ref[slot] = values.T

        def group(g, slot, following):
            cols = columns(g)
            heads_at = pl.multiple_of(g * heads_step, heads_step)
            if first:
                tops = jnp.full((heads_step, queries), LOW, F32)
                sums = jnp.zeros((heads_step, queries), F32)
            else:
                tops = max_in[pl.ds(heads_at, heads_step), :]
                sums = sum_in[pl.ds(heads_at, heads_step), :]
            keys, values = key_ref[slot], value_ref[slot]
            new_tops, new_sums = [], []

            def score(h):
                q = qt_ref[pl.ds(cols + h * head, head), :]
                score_ref[h % DEPTH] = mm(keys[:, h * head : (h + 1) * head], q)

            def soften(h):
                parts = [score_ref[h % DEPTH, j * block : (j + 1) * block, :] for j in range(per_dev)]
                top = tops[h : h + 1, :]
                for j in range(per_dev):
                    peak = jnp.max(parts[j], axis=0, keepdims=True)
                    top = jnp.maximum(top, jnp.where(alive[j], peak, LOW))
                for j in range(per_dev):
                    shift = jnp.where(alive[j], top, -LOW)
                    prob_ref[h % 2, j * block : (j + 1) * block, :] = jnp.exp2(parts[j] - shift).astype(BF)
                new_tops.append(top)

            def mix(h):
                stacked = jnp.concatenate([values[h * head : (h + 1) * head, :], ones], axis=0)
                mixed = mm(stacked, prob_ref[h % 2])
                at = pl.ds(cols + h * head, head)
                if first:
                    new_sums.append(mixed[head : head + 1, :])
                    acc_ref[at, :] = mixed[0:head, :]
                else:
                    fade = jnp.exp2(tops[h : h + 1, :] - new_tops[h])
                    new_sums.append(sums[h : h + 1, :] * fade + mixed[head : head + 1, :])
                    acc_ref[at, :] = acc_in[at, :] * fade + mixed[0:head, :]

            for h in range(DEPTH - 1):
                score(h)
            for h in range(heads_step):
                if h + DEPTH - 1 < heads_step:
                    score(h + DEPTH - 1)
                if h == heads_step // 2 and following is not None:
                    project(following, 1 - slot)
                soften(h)
                if h > 0:
                    mix(h - 1)
            mix(heads_step - 1)
            max_ref[pl.ds(heads_at, heads_step), :] = jnp.concatenate(new_tops, axis=0)
            sum_ref[pl.ds(heads_at, heads_step), :] = jnp.concatenate(new_sums, axis=0)

        groups = width // GROUP_COLS

        def arrive(g):
            if first:
                for load in loads(g):
                    load.wait()

        arrive(0)
        project(0, 0)

        def step_of(i, carry):
            arrive(2 * i + 1)
            group(2 * i, 0, 2 * i + 1)
            pl.when(2 * i + 2 < groups)(lambda: arrive(2 * i + 2))
            group(2 * i + 1, 1, jnp.minimum(2 * i + 2, groups - 1))
            return carry

        lax.fori_loop(0, groups // 2, step_of, 0)

    run()
    if last:
        send_ref[0:width, :] = acc_ref[:, rows:queries]
        send_ref[width : width + H, :] = max_ref[:, rows:queries]
        send_ref[width + H : width + 2 * H, :] = sum_ref[:, rows:queries]


def attend_call(mode, step, pieces, state, where, live, w_qkv, rows, block, peers):
    first, last = mode
    width = w_qkv.shape[0]
    queries = CORES * rows
    stats = jax.ShapeDtypeStruct((H, queries), F32)
    out_shape = [stats, stats, jax.ShapeDtypeStruct((width, queries), F32)]
    scratch = [
        pltpu.VMEM((DEPTH, rows, queries), F32),
        pltpu.VMEM((2, rows, queries), BF),
        pltpu.VMEM((2, rows, GROUP_COLS), BF),
        pltpu.VMEM((2, GROUP_COLS, rows), BF),
    ]
    args = [where, live, *pieces]
    in_specs = [SMEM] * 2 + [VMEM] * len(pieces)
    aliases = {}
    if first:
        args.append(w_qkv)
        in_specs.append(HBM)
        out_shape = [
            jax.ShapeDtypeStruct((width, queries), BF), jax.ShapeDtypeStruct((width, 2 * width), BF), *out_shape
        ]
        scratch += [pltpu.VMEM((width, width), BF), pltpu.SemaphoreType.DMA((width // GROUP_COLS, 3))]
    else:
        args += state
        in_specs += [VMEM] * len(state)
        extra = 1 if last else 0
        at = len(pieces) + 4
        aliases = {at: extra, at + 1: extra + 1, at + 2: extra + 2}
    if last:
        out_shape = [jax.ShapeDtypeStruct((width + 2 * H, rows), F32), *out_shape]
    out = pl.pallas_call(
        functools.partial(attend_kernel, mode, step, len(pieces), rows, block, peers),
        in_specs=in_specs,
        out_specs=[VMEM] * len(out_shape),
        out_shape=out_shape,
        scratch_shapes=scratch,
        input_output_aliases=aliases,
        compiler_params=grant(42 if first else 24),
        cost_estimate=pl.CostEstimate(
            flops=4 * rows * width * width + 16 * rows * queries * width,
            transcendentals=H * rows * queries,
            bytes_accessed=4 << 20,
        ),
    )(*args)
    if first:
        return list(out)
    if last:
        return out
    return [*state[:2], *out]


def pick_row(tile, at):
    rows = lax.broadcasted_iota(jnp.int32, tile.shape, 0)
    return jnp.sum(jnp.where(rows == at, tile.astype(F32), 0.0), axis=0, keepdims=True)


def add_piece(piece_lists, piece_rows, dests, tile, y_own, y_mate, rows, slot, block):
    numbers = lax.broadcasted_iota(jnp.int32, (rows, slot), 0).astype(F32)
    mixes = []
    for dest in range(CORES):
        chosen = jnp.where(numbers == pick_row(piece_lists, dests[dest]), 1.0, 0.0).astype(BF)
        left = jnp.concatenate([tile(dest, j) for j in range(slot // block)], axis=1)
        mixes.append(mm(left, chosen, ((1,), (1,))).astype(BF))
    both = mm(jnp.concatenate(mixes, axis=0), piece_rows)
    y_own[...] += both[0:rows, :]
    y_mate[...] += both[rows:, :]


def add_arrived(step, where, arrived, spread, y_own, y_mate, rows, slot, block, peers):
    me = where[0]
    mate = me + 1 - 2 * (me % CORES)
    source, end = source_of(step, me, peers)
    at = rows // block + source * (slot // block)
    if len(arrived) == 1:
        lists, x = arrived[0][rows:, 0:slot], arrived[0][0:rows, :]
    else:
        lists = jnp.where(end, arrived[1][rows:, 0:slot], arrived[0][rows:, 0:slot])
        x = jnp.where(end, arrived[1][0:rows, :], arrived[0][0:rows, :])
    add_piece(lists, x, (me, mate), lambda dest, j: spread[dest, at + j], y_own, y_mate, rows, slot, block)


def gather_kernel(steps, far_count, rows, slot, far_slot, block, peers, where, nb_own, nb_mate, *refs):
    own, adj_own, adj_mate, *refs = refs
    count = sum(steps)
    arrived = refs[:count]
    far = refs[count : count + far_count]
    y_own, y_mate, spread = refs[count + far_count :]
    me, cluster = where[0], where[1]
    mate = me + 1 - 2 * (me % CORES)
    spread[...] = jnp.zeros(spread.shape, BF)
    per_dev, tiles = adj_own.shape[0], adj_own.shape[1]
    for dest, (adj, nb) in enumerate(((adj_own, nb_own), (adj_mate, nb_mate))):
        for b in range(per_dev):
            for s in range(tiles):
                spread[dest, nb[b, s], b * block : (b + 1) * block, :] = adj[b, s]
    mine = jnp.concatenate([spread[0, j] for j in range(per_dev)], axis=1)
    y_own[...] = mm(mine, own[0:rows, :])
    y_mate[...] = jnp.zeros(y_mate.shape, F32)
    base = rows // block
    add_piece(
        own[rows:, 0:slot], own[0:rows, :], (me, mate),
        lambda dest, j: spread[dest, base + me * (slot // block) + j],
        y_own, y_mate, rows, slot, block,
    )
    first_far = base + peers * (slot // block)
    tiles_far = []
    for f in range(far_count):
        source = far_source(f, cluster, far_count)
        for j in range(far_slot // block):
            tiles_far.append(spread[0, first_far + source * (far_slot // block) + j])
    y_own[...] += mm(jnp.concatenate(tiles_far, axis=1), jnp.concatenate([r[...] for r in far], axis=0))
    at = 0
    for step, width in enumerate(steps):
        add_arrived(step + 1, where, arrived[at : at + width], spread, y_own, y_mate, rows, slot, block, peers)
        at += width


def gather_more_kernel(step, count, rows, slot, block, peers, where, *refs):
    arrived = refs[:count]
    spread, own_in, mate_in, y_own, y_mate = refs[count:]
    y_own[...] = own_in[...]
    y_mate[...] = mate_in[...]
    add_arrived(step, where, arrived, spread, y_own, y_mate, rows, slot, block, peers)


def far_source(step, cluster, clusters):
    if clusters & (clusters - 1) == 0:
        return cluster ^ step
    return (cluster - step) % clusters


def far_target(step, cluster, clusters):
    if clusters & (clusters - 1) == 0:
        return cluster ^ step
    return (cluster + step) % clusters


def pack_kernel(lists, x, out, sem):
    rows = x.shape[0]
    load = pltpu.make_async_copy(x, out.at[0:rows, :], sem)
    load.start()
    peers, slot = lists.shape[1:]
    numbers = lists[0].astype(F32).astype(BF)
    if slot < out.shape[1]:
        numbers = jnp.concatenate([numbers, jnp.zeros((peers, out.shape[1] - slot), BF)], axis=1)
    out[rows : rows + peers, :] = numbers
    load.wait()


def pick_kernel(clusters, rows, where, lists, x, *outs):
    numbers = lax.broadcasted_iota(jnp.int32, (rows, lists.shape[-1]), 0)
    for step, out in enumerate(outs):
        row = lists[0, pl.ds(far_target(step, where[1], clusters), 1), :]
        chosen = jnp.where(numbers == row, 1.0, 0.0).astype(BF)
        out[...] = mm(chosen, x[0:rows, :], ((0,), (0,))).astype(BF)


def local_kernel(x, y_own, y_got, w, out):
    mixed = (y_own[...] + y_got[...]).astype(BF)
    agg = mm(mixed, w[...])
    out[...] = layer_norm(x[...].astype(F32) + agg)


def tail_kernel(rows, x, local, top, total, acc, got, w_out, w_up_all, w_down, out, w_up, sem):
    load = pltpu.make_async_copy(w_up_all, w_up, sem)
    load.start()
    heads = top.shape[0]
    width = acc.shape[0]
    head = width // heads
    top_a = top[:, 0:rows]
    top_b = got[width : width + heads, :]
    peak = jnp.maximum(top_a, top_b)
    fade_a = jnp.exp2(top_a - peak)
    fade_b = jnp.exp2(top_b - peak)
    whole = total[:, 0:rows] * fade_a + got[width + heads :, :] * fade_b
    fade_a = fade_a / whole
    fade_b = fade_b / whole
    pieces = []
    for h in range(heads):
        at = slice(h * head, (h + 1) * head)
        pieces.append((acc[at, 0:rows] * fade_a[h : h + 1, :] + got[at, :] * fade_b[h : h + 1, :]).astype(BF))
    attended = jnp.concatenate(pieces, axis=0)
    projected = mm(attended, w_out[...], ((0,), (0,)))
    summed = local[...] + layer_norm(x[...].astype(F32) + projected)
    load.wait()
    activated = jax.nn.gelu(mm(summed.astype(BF), w_up[...])).astype(BF)
    out[...] = layer_norm(summed + mm(activated, w_down[...])).astype(BF)


def line_plan(
    node_feats,
    w_gcn,
    adj_tiles,
    neighbor_blocks,
    inner_rows,
    outer_rows,
    w_qkv,
    key_blocks,
    key_counts,
    w_out,
    w_up,
    w_down,
):
    rows, width = node_feats.shape
    block = adj_tiles.shape[-1]
    peers = lax.axis_size("dev")
    clusters = lax.axis_size("group")
    chips = peers // CORES
    slot = inner_rows.shape[-1]
    far_slot = outer_rows.shape[-1]
    cluster = lax.axis_index("group")
    where = jnp.stack([lax.axis_index("dev"), cluster]).astype(jnp.int32)
    swap = [(CORES * c + k, CORES * c + 1 - k) for c in range(chips) for k in range(CORES)]

    def cross(value, pairs):
        lanes = [(CORES * a + k, CORES * b + k) for a, b in pairs for k in range(CORES)]
        return lax.ppermute(value, "dev", lanes)

    piece = pl.pallas_call(
        pack_kernel,
        in_specs=[VMEM, HBM],
        out_specs=VMEM,
        out_shape=jax.ShapeDtypeStruct((rows + peers, width), BF),
        scratch_shapes=[pltpu.SemaphoreType.DMA],
        compiler_params=grant(4),
        name="pack",
    )(inner_rows, node_feats)
    outer, middle = [(0, 1), (1, 0), (2, 3), (3, 2)], [(1, 2), (2, 1)]
    outward = [(1, 0), (2, 3)]
    near = cross(piece, outer)
    mid = cross(piece, middle)
    mate_piece = lax.ppermute(piece, "dev", swap)
    mate_adj = lax.ppermute(adj_tiles, "dev", swap)
    mate_nb = lax.ppermute(neighbor_blocks, "dev", swap)

    picked = pl.pallas_call(
        functools.partial(pick_kernel, clusters, rows),
        in_specs=[SMEM, VMEM, VMEM],
        out_specs=[VMEM] * clusters,
        out_shape=[jax.ShapeDtypeStruct((far_slot, width), BF)] * clusters,
        compiler_params=grant(8),
        cost_estimate=pl.CostEstimate(
            flops=2 * rows * clusters * far_slot * width, transcendentals=0, bytes_accessed=1 << 20
        ),
        name="pick",
    )(where, outer_rows, piece)
    far = [picked[0]]
    for s in range(1, clusters):
        pairs = [(c, far_target(s, c, clusters)) for c in range(clusters)]
        far.append(lax.ppermute(picked[s], "group", pairs))

    slots = jnp.arange(key_blocks.shape[1], dtype=jnp.int32)[None, :]
    live = jnp.sum(jnp.where(slots < key_counts[:, None], jnp.left_shift(1, key_blocks), 0), axis=1)
    live = live.astype(jnp.int32)

    attend = lambda step, pieces, state, last=False: attend_call(
        (step == 0, last), step, pieces, state, where, live, w_qkv, rows, block, peers
    )
    state = attend(0, [piece, mate_piece], None)
    near, mid, to_far, state[2] = lax.optimization_barrier((near, mid, piece, state[2]))
    ends = cross(to_far, [(0, 3), (3, 0)])
    to_end = cross(mid, outward)
    to_mid = cross(near, middle)
    state = attend(1, [near], state)
    state = attend(2, [mid, ends], state)
    sums = gather_call(
        where, neighbor_blocks, mate_nb, piece, adj_tiles, mate_adj, [near, mid, ends], (1, 2), far,
        rows, slot, far_slot, block, peers,
    )
    sums = gather_more_call(3, where, [to_mid, to_end], sums, rows, slot, block, peers)
    y_send, state[2] = lax.optimization_barrier((sums[1], state[2]))
    y_got = lax.ppermute(y_send, "dev", swap)
    send, top, total, acc = attend(3, [to_mid, to_end], state, True)
    got = lax.ppermute(send, "dev", swap)
    local = pl.pallas_call(
        local_kernel,
        in_specs=[VMEM] * 4,
        out_specs=VMEM,
        out_shape=jax.ShapeDtypeStruct((rows, width), F32),
        compiler_params=grant(16),
        cost_estimate=pl.CostEstimate(flops=2 * rows * width * width, transcendentals=0, bytes_accessed=4 << 20),
        name="local",
    )(node_feats, sums[0], y_got, w_gcn)
    return pl.pallas_call(
        functools.partial(tail_kernel, rows),
        in_specs=[VMEM] * 7 + [HBM, VMEM],
        out_specs=VMEM,
        out_shape=jax.ShapeDtypeStruct((rows, width), BF),
        scratch_shapes=[pltpu.VMEM(w_up.shape, BF), pltpu.SemaphoreType.DMA],
        compiler_params=grant(32),
        cost_estimate=pl.CostEstimate(
            flops=2 * rows * width * (width + 2 * w_up.shape[1]), transcendentals=0, bytes_accessed=12 << 20
        ),
        name="tail",
    )(node_feats, local, top, total, acc, got, w_out, w_up, w_down)


def gather_call(
    where, nb_own, nb_mate, own, adj_own, adj_mate, arrived, steps, far, rows, slot, far_slot, block, peers
):
    width = own.shape[1]
    table_blocks = (rows + peers * slot + len(far) * far_slot) // block
    y = jax.ShapeDtypeStruct((rows, width), F32)
    spread = jax.ShapeDtypeStruct((CORES, table_blocks, rows, block), BF)
    return pl.pallas_call(
        functools.partial(gather_kernel, steps, len(far), rows, slot, far_slot, block, peers),
        in_specs=[SMEM] * 3 + [VMEM] * (3 + len(arrived) + len(far)),
        out_specs=[VMEM] * 3,
        out_shape=[y, y, spread],
        compiler_params=grant(24),
        cost_estimate=pl.CostEstimate(
            flops=4 * rows * rows * width * (2 + len(steps)), transcendentals=0, bytes_accessed=8 << 20
        ),
        name="gather",
    )(where, nb_own, nb_mate, own, adj_own, adj_mate, *arrived, *far)


def gather_more_call(step, where, pair, sums, rows, slot, block, peers):
    y_own, y_mate, spread = sums
    return pl.pallas_call(
        functools.partial(gather_more_kernel, step, len(pair), rows, slot, block, peers),
        in_specs=[SMEM] + [VMEM] * (len(pair) + 3),
        out_specs=[VMEM] * 2,
        out_shape=[jax.ShapeDtypeStruct(y_own.shape, F32)] * 2,
        input_output_aliases={2 + len(pair): 0, 3 + len(pair): 1},
        compiler_params=grant(16),
        cost_estimate=pl.CostEstimate(
            flops=4 * rows * rows * y_own.shape[1], transcendentals=0, bytes_accessed=4 << 20
        ),
        name="gather_more",
    )(where, *pair, spread, y_own, y_mate)


def per_device(*args):
    inner, feats, tiles = args[4], args[0], args[2]
    whole_slots = inner.shape[-1] == feats.shape[0] and feats.shape[0] <= 256
    whole_slots = whole_slots and args[8].shape[0] <= 31
    if whole_slots and lax.axis_size("dev") == 4 * CORES and inner.shape[-1] % tiles.shape[-1] == 0:
        return line_plan(*args)
    return gathered_plan(*args)


def solution(mesh):
    placed = (
        P(("group", "dev"), None),
        P(),
        P(("group", "dev"), None, None, None),
        P(("group", "dev"), None),
        P(("group", "dev"), None, None),
        P(("group", "dev"), None, None),
        P(),
        P("group", None),
        P("group"),
        P(),
        P(),
        P(),
    )
    return jax.shard_map(per_device, mesh=mesh, in_specs=placed, out_specs=P(("group", "dev"), None), check_vma=False)
```
